8 devices in a mesh: dp: 1 (over z), tp: 2 (over y), sp: 4 (over x, core).
Axes of the slice: x: 2, y: 2, z: 1, core: 2. Of those that a mesh axis runs over, the one named last changes fastest.
Arguments:
- hidden: bfloat16 [128, 2880], P('dp')
- seq_lens: int32 [128], P('dp')
- rope_cos: float32 [128, 32], P('dp')
- rope_sin: float32 [128, 32], P('dp')
- k_cache: bfloat16 [128, 512, 8, 64], P('dp', 'sp', 'tp')
- v_cache: bfloat16 [128, 512, 8, 64], P('dp', 'sp', 'tp')
- norm_gain: bfloat16 [2880], replicated
- w_qkv: bfloat16 [2880, 8, 640], P(None, 'tp')
- b_qkv: bfloat16 [8, 640], P('tp')
- sink_logits: float32 [64], P('tp')
- w_o: bfloat16 [4096, 2880], P('tp')
- b_o: bfloat16 [2880], replicated
Outputs:
- output 1: bfloat16 [128, 2880], P('dp')
- output 2: bfloat16 [128, 512, 8, 64], P('dp', 'sp', 'tp')
- output 3: bfloat16 [128, 512, 8, 64], P('dp', 'sp', 'tp')
All inputs are finite; a program needn't handle non-finite values.
Results may differ from the reference program's by a relative error of at most 0.00539607.
Values sent between devices are 32-bit elements.
A program may use at most 1 GiB of HBM per device.

```python
import math
import jax
import jax.numpy as jnp
from jax import lax

D_MODEL = 2880
Q_HEADS = 64
KV_HEADS = 8
HEAD_DIM = 64
SEQ_COUNT = 128
CTX_LEN = 512
ROPE_BASE = 150000
NORM_EPS = 1e-5


def rotate_half(heads_in, cos_part, sin_part):
    half_dim = heads_in.shape[-1] // 2
    first_half = heads_in[..., :half_dim]
    second_half = heads_in[..., half_dim:]
    return jnp.concatenate([first_half * cos_part - second_half * sin_part, second_half * cos_part + first_half * sin_part], axis=-1)


def setup_inputs(seed: int = 0, part: int = 0) -> dict:
    shared_keys = jax.random.split(jax.random.key(seed), 6)
    part_keys = jax.random.split(jax.random.fold_in(jax.random.key(seed + 1), part), 5)
    group_size = Q_HEADS // KV_HEADS
    qkv_width = (group_size + 2) * HEAD_DIM
    key_scale = math.sqrt(math.log(CTX_LEN) / 2.0)
    sink_center = math.log(CTX_LEN / 2.0) + 0.6 * key_scale * key_scale - 1.0
    hidden = (0.5 * jax.random.normal(part_keys[0], (SEQ_COUNT, D_MODEL), jnp.float32)).astype(jnp.bfloat16)
    drawn_lens = jax.random.randint(part_keys[1], (SEQ_COUNT,), 0, CTX_LEN, jnp.int32)
    full_row = jax.random.randint(part_keys[2], (), 0, SEQ_COUNT, jnp.int32)
    seq_lens = jnp.where(jnp.arange(SEQ_COUNT) == full_row, CTX_LEN - 1, drawn_lens).astype(jnp.int32)
    inv_freq = jnp.exp(jnp.arange(HEAD_DIM // 2, dtype=jnp.float32) * (-2.0 * math.log(ROPE_BASE) / HEAD_DIM))
    angles = seq_lens.astype(jnp.float32)[:, None] * inv_freq[None, :]
    cache_shape = (SEQ_COUNT, CTX_LEN, KV_HEADS, HEAD_DIM)
    k_cache = (key_scale * jax.random.normal(part_keys[3], cache_shape, jnp.float32)).astype(jnp.bfloat16)
    v_cache = jax.random.normal(part_keys[4], cache_shape, jnp.float32).astype(jnp.bfloat16)
    norm_gain = (1.0 + 0.2 * jax.random.normal(shared_keys[0], (D_MODEL,), jnp.float32)).astype(jnp.bfloat16)
    w_qkv = (D_MODEL ** -0.5 * jax.random.normal(shared_keys[1], (D_MODEL, KV_HEADS, qkv_width), jnp.float32)).astype(jnp.bfloat16)
    b_qkv = (0.5 * jax.random.normal(shared_keys[2], (KV_HEADS, qkv_width), jnp.float32)).astype(jnp.bfloat16)
    sink_logits = sink_center + jax.random.normal(shared_keys[3], (Q_HEADS,), jnp.float32)
    w_o = (4.0 * (Q_HEADS * HEAD_DIM) ** -0.5 * jax.random.normal(shared_keys[4], (Q_HEADS * HEAD_DIM, D_MODEL), jnp.float32)).astype(jnp.bfloat16)
    b_o = (0.3 * jax.random.normal(shared_keys[5], (D_MODEL,), jnp.float32)).astype(jnp.bfloat16)
    return {"hidden": hidden, "seq_lens": seq_lens, "rope_cos": jnp.cos(angles), "rope_sin": jnp.sin(angles), "k_cache": k_cache, "v_cache": v_cache, "norm_gain": norm_gain, "w_qkv": w_qkv, "b_qkv": b_qkv, "sink_logits": sink_logits, "w_o": w_o, "b_o": b_o}


def reference(hidden, seq_lens, rope_cos, rope_sin, k_cache, v_cache, norm_gain, w_qkv, b_qkv, sink_logits, w_o, b_o):
    group_size = Q_HEADS // KV_HEADS
    x_wide = hidden.astype(jnp.float32)
    inv_rms = lax.rsqrt(jnp.mean(x_wide * x_wide, axis=-1, keepdims=True) + NORM_EPS)
    normed = (x_wide * inv_rms * norm_gain.astype(jnp.float32)).astype(jnp.bfloat16)
    qkv_all = jnp.dot(normed, w_qkv.reshape(D_MODEL, KV_HEADS * (group_size + 2) * HEAD_DIM), preferred_element_type=jnp.float32)
    qkv_all = (qkv_all + b_qkv.astype(jnp.float32).reshape(-1)).reshape(SEQ_COUNT, KV_HEADS, group_size + 2, HEAD_DIM)
    q_rot = rotate_half(qkv_all[:, :, :group_size], rope_cos[:, None, None, :], rope_sin[:, None, None, :]).astype(jnp.bfloat16)
    k_new = rotate_half(qkv_all[:, :, group_size], rope_cos[:, None, :], rope_sin[:, None, :]).astype(jnp.bfloat16)
    v_new = qkv_all[:, :, group_size + 1].astype(jnp.bfloat16)
    positions = jnp.arange(CTX_LEN)
    is_new = (positions[None, :] == seq_lens[:, None])[:, :, None, None]
    k_out = jnp.where(is_new, k_new[:, None], k_cache)
    v_out = jnp.where(is_new, v_new[:, None], v_cache)
    sink_kg = sink_logits.reshape(KV_HEADS, group_size)
    logit_scale = HEAD_DIM ** -0.5

    def one_sequence(per_seq):
        q_seq, k_seq, v_seq, len_seq = per_seq
        logits = jnp.einsum("kgd,lkd->kgl", q_seq.astype(jnp.float32), k_seq.astype(jnp.float32)) * logit_scale
        logits = jnp.where((positions <= len_seq)[None, None, :], logits, -jnp.inf)
        row_max = jnp.maximum(jnp.max(logits, axis=-1), sink_kg)
        weights = jnp.exp(logits - row_max[..., None])
        denominator = jnp.sum(weights, axis=-1) + jnp.exp(sink_kg - row_max)
        weighted = jnp.einsum("kgl,lkd->kgd", weights.astype(jnp.bfloat16).astype(jnp.float32), v_seq.astype(jnp.float32))
        return weighted / denominator[..., None]

    head_out = lax.map(one_sequence, (q_rot, k_out, v_out, seq_lens))
    attn_out = jnp.dot(head_out.astype(jnp.bfloat16).reshape(SEQ_COUNT, Q_HEADS * HEAD_DIM), w_o, preferred_element_type=jnp.float32)
    out_hidden = (x_wide + attn_out + b_o.astype(jnp.float32)).astype(jnp.bfloat16)
    return out_hidden, k_out, v_out
```

```python
import functools
import jax
import jax.numpy as jnp
from jax import lax
from jax.sharding import PartitionSpec as P
from jax.experimental import pallas as pl
from jax.experimental.pallas import tpu as pltpu

NORM_EPS = 1e-5
CHUNK = 8
GROUP = 32
ROWS = 512
MESH = pl.DeviceIdType.MESH


def attend_kernel(lens_hbm, sinks_hbm, x_hbm, gain_hbm, w_hbm, b_hbm, cos_hbm, sin_hbm, k_hbm, v_hbm,
                  k_out, v_out, part,
                  lens, sinks, x_t, gain, b_qkv, cos_t, sin_t,
                  w_buf, w_f32, acc, h_buf, q_buf, kn_t, vn_t, k_buf, v_buf, e_buf,
                  small_sem, w_sem, in_sem, out_sem):
    d_model, seqs = x_t.shape
    n_chunks = seqs // CHUNK
    n_full, tail = divmod(d_model, ROWS)

    smalls = [pltpu.make_async_copy(src, dst, small_sem.at[i]) for i, (src, dst) in enumerate(
        [(x_hbm, x_t), (gain_hbm, gain), (b_hbm, b_qkv), (cos_hbm, cos_t), (sin_hbm, sin_t), (lens_hbm, lens), (sinks_hbm, sinks)])]
    for c in smalls:
        c.start()

    def w_copies(i, n):
        rows = pl.ds(i * ROWS, n)
        return [pltpu.make_async_copy(w_hbm.at[rows, :, pl.ds(c * 128, 128)], w_buf.at[c, rows], w_sem.at[i, c]) for c in range(5)]

    for i in range(n_full):
        for c in w_copies(i, ROWS):
            c.start()
    for c in w_copies(n_full, tail):
        c.start()

    def cache_in(a, i):
        rows = pl.ds(i * CHUNK, CHUNK)
        src, dst = ((k_hbm, k_buf), (v_hbm, v_buf))[a]
        return pltpu.make_async_copy(src.at[rows], dst.at[rows], in_sem.at[a, i])

    def cache_out(a, i):
        rows = pl.ds(i * CHUNK, CHUNK)
        src, dst = ((k_buf, k_out), (v_buf, v_out))[a]
        return pltpu.make_async_copy(src.at[rows], dst.at[rows], out_sem.at[a, i])

    for c in smalls:
        c.wait()

    sq = jnp.zeros((seqs, 1), jnp.float32)
    xs = []
    for j in range(0, d_model, 128):
        n = min(128, d_model - j)
        xb = x_t[j:j + n, :].astype(jnp.float32).T
        xs.append(xb)
        sq = sq + jnp.sum(xb * xb, axis=1, keepdims=True)
    inv = lax.rsqrt(sq * (1.0 / d_model) + NORM_EPS)
    for i, j in enumerate(range(0, d_model, 128)):
        n = min(128, d_model - j)
        h_buf[:, j:j + n] = (xs[i] * inv * gain[0:1, j:j + n]).astype(jnp.bfloat16)

    bias = b_qkv[...].astype(jnp.float32)
    for p in range(2):
        for c in range(5):
            for u in range(2):
                acc[p, c, :, u * 128:u * 128 + 128] = jnp.broadcast_to(bias[2 * p + u:2 * p + u + 1, c * 128:c * 128 + 128], (seqs, 128))

    def project(i, n):
        rows = pl.multiple_of(i * ROWS, ROWS)
        h = h_buf[:, pl.ds(rows, n)]
        for c, copy in enumerate(w_copies(i, n)):
            copy.wait()
        for c in range(5):
            w_f32[c, 0:4 * n, :] = w_buf[c, pl.ds(rows, n)].reshape(4 * n, 128).astype(jnp.float32)
            for p in range(2):
                w = jnp.concatenate([w_f32[c, pl.ds(2 * p + u, n, stride=4), :].astype(jnp.bfloat16) for u in range(2)], axis=1)
                acc[p, c] += jnp.dot(h, w, preferred_element_type=jnp.float32)

    def project_step(i, carry):
        project(i, ROWS)

        @pl.when(i == 2)
        def _():
            for ch in range(n_chunks):
                cache_in(0, ch).start()

        @pl.when(i == 4)
        def _():
            for ch in range(n_chunks):
                cache_in(1, ch).start()
        return carry

    lax.fori_loop(0, n_full, project_step, 0)
    project(n_full, tail)

    lane = lax.broadcasted_iota(jnp.int32, (seqs, 128), 1)
    low = lane < 64
    first_half = (lane & 63) < 32
    cos4 = jnp.concatenate([cos_t[...]] * 4, axis=0).T
    sin4 = jnp.concatenate([sin_t[...]] * 4, axis=0).T
    sin4 = jnp.where(first_half, -sin4, sin4)

    def rotate(t):
        other = jnp.where(first_half, pltpu.roll(t, 96, 1), pltpu.roll(t, 32, 1))
        return t * cos4 + other * sin4

    for p in range(2):
        lanes = slice(p * 128, p * 128 + 128)
        for tile in range(5):
            t0 = acc[p, tile, :, 0:128]
            t1 = acc[p, tile, :, 128:256]
            even = jnp.where(low, t0, pltpu.roll(t1, 64, 1))
            odd = jnp.where(low, pltpu.roll(t0, 64, 1), t1)
            if tile < 4:
                q_buf[p, pl.ds(2 * tile, seqs, stride=8), :] = rotate(even)
                q_buf[p, pl.ds(2 * tile + 1, seqs, stride=8), :] = rotate(odd)
            else:
                kn_t[lanes, :] = rotate(even).T
                vn_t[lanes, :] = odd.T

    base = lax.axis_index("sp") * 128
    lane8 = lax.broadcasted_iota(jnp.int32, (8, 128), 1)
    row8 = lax.broadcasted_iota(jnp.int32, (8, 128), 0)
    sink_rows = []
    for k in range(4):
        t = jnp.zeros((8, 128), jnp.float32)
        for g in range(8):
            t = jnp.where(row8 == g, sinks[k * 8 + g], t)
        sink_rows.append(t)
    sink_col = jnp.concatenate(sink_rows, axis=0)[:, 0:1]
    lane32 = lax.broadcasted_iota(jnp.int32, (32, 128), 1)
    lane256 = lax.broadcasted_iota(jnp.int32, (256, 128), 1)
    q_lane = lax.broadcasted_iota(jnp.int32, (8, 256), 1) // 64
    half8 = lane8 < 64

    def put_new(buf, new_t, i):
        for u in range(CHUNK):
            b = i * CHUNK + u
            loc = lens[b] - base

            @pl.when((loc >= 0) & (loc < 128))
            def _():
                shift = lax.rem(loc - b + 256, 128)
                buf[b] = jnp.where(lane256 == loc, pltpu.roll(new_t[...], shift, 1), buf[b].astype(jnp.float32)).astype(jnp.bfloat16)

    def score_step(i, carry):
        cache_in(0, i).wait()
        put_new(k_buf, kn_t, i)
        cache_out(0, i).start()
        group = i // (GROUP // CHUNK)
        m_acc = part[group, 256:264, 0:128]
        s_acc = part[group, 256:264, 128:256]
        for u in range(CHUNK):
            b = i * CHUNK + u
            j = lax.rem(i, GROUP // CHUNK) * CHUNK + u
            rows = jnp.concatenate([q_buf[p, pl.ds(pl.multiple_of(b * 8, 8), 8), :] for p in range(2)], axis=1)
            q_blk = jnp.concatenate([jnp.where(q_lane == k, rows, 0.0) for k in range(4)], axis=0).astype(jnp.bfloat16)
            logits = jnp.dot(q_blk, k_buf[b], preferred_element_type=jnp.float32) * 0.125
            logits = jnp.where(lane32 <= lens[b] - base, logits, -jnp.inf)
            m = jnp.maximum(jnp.max(logits, axis=1, keepdims=True), sink_col)
            e = jnp.exp(logits - m)
            s = jnp.sum(e, axis=1, keepdims=True)
            e_buf[pl.ds(pl.multiple_of(b * 32, 32), 32), :] = e.astype(jnp.bfloat16)
            for k in range(4):
                here = lane8 == j * 4 + k
                m_acc = jnp.where(here, m[8 * k:8 * k + 8], m_acc)
                s_acc = jnp.where(here, s[8 * k:8 * k + 8], s_acc)
        part[group, 256:264, 0:128] = m_acc
        part[group, 256:264, 128:256] = s_acc
        return carry

    lax.fori_loop(0, n_chunks, score_step, 0)

    def value_step(i, carry):
        cache_in(1, i).wait()
        put_new(v_buf, vn_t, i)
        cache_out(1, i).start()
        group = i // (GROUP // CHUNK)
        for u in range(CHUNK):
            b = i * CHUNK + u
            j = lax.rem(i, GROUP // CHUNK) * CHUNK + u
            e = e_buf[pl.ds(pl.multiple_of(b * 32, 32), 32), :]
            r = lax.dot_general(e, v_buf[b], (((1,), (1,)), ((), ())), preferred_element_type=jnp.float32)
            rows = pl.ds(pl.multiple_of(j * 8, 8), 8)
            part[group, rows, 0:128] = jnp.where(half8, r[0:8, 0:128], r[8:16, 0:128])
            part[group, rows, 128:256] = jnp.where(half8, r[16:24, 128:256], r[24:32, 128:256])
        return carry

    lax.fori_loop(0, n_chunks, value_step, 0)

    def drain(i, carry):
        cache_out(0, i).wait()
        cache_out(1, i).wait()
        return carry

    lax.fori_loop(0, n_chunks, drain, 0)


def local_attention(hidden, seq_lens, rope_cos, rope_sin, k_cache, v_cache, norm_gain, w_qkv, b_qkv, sink_logits):
    seqs, d_model = hidden.shape
    ctx, kv, dim = k_cache.shape[1:]
    k_t = k_cache.transpose(0, 2, 3, 1).reshape(seqs, kv * dim, ctx)
    v_t = v_cache.transpose(0, 2, 3, 1).reshape(seqs, kv * dim, ctx)
    hbm = lambda a: pltpu.with_memory_space_constraint(a, pltpu.HBM)
    vmem = pl.BlockSpec(memory_space=pltpu.VMEM)
    anyw = pl.BlockSpec(memory_space=pltpu.HBM)
    n_chunks = seqs // CHUNK
    k_out, v_out, part = pl.pallas_call(
        attend_kernel,
        out_shape=(jax.ShapeDtypeStruct(k_t.shape, k_t.dtype), jax.ShapeDtypeStruct(v_t.shape, v_t.dtype),
                   jax.ShapeDtypeStruct((seqs // GROUP, GROUP * 8 + 8, kv * dim), jnp.float32)),
        in_specs=[anyw] * 10,
        out_specs=(anyw, anyw, vmem),
        scratch_shapes=[
            pltpu.SMEM((seqs,), jnp.int32),
            pltpu.SMEM((kv * 8,), jnp.float32),
            pltpu.VMEM((d_model, seqs), jnp.bfloat16),
            pltpu.VMEM((1, d_model), jnp.float32),
            pltpu.VMEM(b_qkv.shape, jnp.bfloat16),
            pltpu.VMEM((dim // 2, seqs), jnp.float32),
            pltpu.VMEM((dim // 2, seqs), jnp.float32),
            pltpu.VMEM((5, d_model, kv, 128), jnp.bfloat16),
            pltpu.VMEM((5, ROWS * kv, 128), jnp.float32),
            pltpu.VMEM((2, 5, seqs, 256), jnp.float32),
            pltpu.VMEM((seqs, 2944), jnp.bfloat16),
            pltpu.VMEM((2, seqs * 8, 128), jnp.float32),
            pltpu.VMEM((kv * dim, seqs), jnp.float32),
            pltpu.VMEM((kv * dim, seqs), jnp.float32),
            pltpu.VMEM(k_t.shape, jnp.bfloat16),
            pltpu.VMEM(v_t.shape, jnp.bfloat16),
            pltpu.VMEM((seqs * 32, 128), jnp.bfloat16),
            pltpu.SemaphoreType.DMA((7,)),
            pltpu.SemaphoreType.DMA((6, 5)),
            pltpu.SemaphoreType.DMA((2, n_chunks)),
            pltpu.SemaphoreType.DMA((2, n_chunks)),
        ],
        compiler_params=pltpu.CompilerParams(vmem_limit_bytes=56 * 1024 * 1024),
        cost_estimate=pl.CostEstimate(flops=3 * 10**9, bytes_accessed=48 * 10**6, transcendentals=10**6),
    )(hbm(seq_lens), hbm(sink_logits), hbm(hidden.T), norm_gain.astype(jnp.float32)[None, :], hbm(w_qkv), hbm(b_qkv),
      hbm(rope_cos.T), hbm(rope_sin.T), hbm(k_t), hbm(v_t))
    back = lambda a: a.reshape(seqs, kv, dim, ctx).transpose(0, 3, 1, 2)
    return back(k_out), back(v_out), part


COLS = 512
HALF = 3 * COLS


def exchange_kernel(part, sinks_hbm, bias, w_hbm, y_out,
                    sinks, w_buf, from_core, to_chip, own, from_chip, o_buf, lhs, y_buf, from_tp, gather,
                    small_sem, w_sem, core_send, core_recv, chip_send, chip_recv, tp_send, tp_recv, ag_send, ag_recv):
    tp = lax.axis_index("tp")
    sp = lax.axis_index("sp")
    core = lax.rem(sp, 2)
    chip = sp // 2
    d_out = w_hbm.shape[0]
    n_cols = [(n, min(COLS, d_out - n)) for n in range(0, d_out, COLS)]
    sibling = {"sp": sp + 1 - 2 * core}
    across_x = {"sp": lax.rem(sp + 2, 4)}
    across_y = {"tp": 1 - tp}

    small = pltpu.make_async_copy(sinks_hbm, sinks, small_sem)
    small.start()
    w_copies = [pltpu.make_async_copy(w_hbm.at[pl.ds(n, w)], w_buf.at[pl.ds(n, w)], w_sem.at[i]) for i, (n, w) in enumerate(n_cols)]
    for c in w_copies:
        c.start()

    barrier = pltpu.get_barrier_semaphore()
    for peer in (sibling, across_x, across_y):
        pl.semaphore_signal(barrier, inc=1, device_id=peer, device_id_type=MESH)
    pl.semaphore_wait(barrier, 3)

    def remote(src, dst, ss, rs, peer):
        return pltpu.make_async_remote_copy(src_ref=src, dst_ref=dst, send_sem=ss, recv_sem=rs, device_id=peer, device_id_type=MESH)

    core_copies = []
    for r in range(2):
        x_side = (1 - chip) if r == 0 else chip
        group = 2 * x_side + (1 - core)
        core_copies.append(remote(part.at[group], from_core.at[r], core_send.at[r], core_recv.at[r], sibling))
    for c in core_copies:
        c.start()

    lane = lax.broadcasted_iota(jnp.int32, (8, 128), 1)
    row = lax.broadcasted_iota(jnp.int32, (8, 128), 0)
    high = lane // 64

    def spread(f, j, p):
        return jnp.take_along_axis(f, j * 4 + 2 * p + high, axis=1)

    def stats(a, b):
        m_a, s_a = a[0], a[1]
        m_b, s_b = b[0], b[1]
        m = jnp.maximum(m_a, m_b)
        f_a = jnp.exp(m_a - m)
        f_b = jnp.exp(m_b - m)
        return m, s_a * f_a + s_b * f_b, f_a, f_b

    def stat_rows(ref):
        return ref[256:264, 0:128], ref[256:264, 128:256]

    def merge(a_ref, b_ref, out_ref, f_a, f_b, j0, j1):
        for j in range(j0, j1):
            rows = slice(8 * j, 8 * j + 8)
            for p in range(2):
                cols = slice(128 * p, 128 * p + 128)
                out_ref[rows, cols] = a_ref[rows, cols] * spread(f_a, j, p) + b_ref[rows, cols] * spread(f_b, j, p)

    pieces = [(0, 8), (8, 16), (16, 24), (24, 32)]

    def piece_rows(i):
        j0, j1 = pieces[i]
        return pl.ds(8 * j0, 8 * (j1 - j0) + (8 if i == len(pieces) - 1 else 0))

    core_copies[0].wait_recv()
    away = part.at[2 * (1 - chip) + core]
    m, s, f_a, f_b = stats(stat_rows(away), stat_rows(from_core.at[0]))
    to_chip[256:264, 0:128] = m
    to_chip[256:264, 128:256] = s
    chip_copies = [remote(to_chip.at[piece_rows(i)], from_chip.at[piece_rows(i)], chip_send.at[i], chip_recv.at[i], across_x) for i in range(len(pieces))]
    order = [3, 0, 1, 2]
    for i in order:
        merge(away, from_core.at[0], to_chip, f_a, f_b, *pieces[i])
        chip_copies[i].start()

    core_copies[1].wait_recv()
    here = part.at[2 * chip + core]
    m_own, s_own, f_a, f_b = stats(stat_rows(here), stat_rows(from_core.at[1]))
    merge(here, from_core.at[1], own, f_a, f_b, 0, 32)

    small.wait()
    sink = jnp.zeros((8, 128), jnp.float32)
    k_of_lane = lane & 3
    for k in range(4):
        for g in range(8):
            sink = jnp.where((row == g) & (k_of_lane == k), sinks[k * 8 + g], sink)

    chip_copies[3].wait_recv()
    m, s, f_a, f_b = stats((m_own, s_own), stat_rows(from_chip))
    scale = 1.0 / (s + jnp.exp(sink - m))
    f_a = f_a * scale
    f_b = f_b * scale
    for i in order:
        if i != 3:
            chip_copies[i].wait_recv()
        for j in range(*pieces[i]):
            rows = slice(8 * j, 8 * j + 8)
            for p in range(2):
                cols = slice(128 * p, 128 * p + 128)
                o_buf[p, rows, :] = own[rows, cols] * spread(f_a, j, p) + from_chip[rows, cols] * spread(f_b, j, p)

    low = lax.broadcasted_iota(jnp.int32, (32, 128), 1) < 64
    for p in range(2):
        for t in range(4):
            a = o_buf[p, pl.ds(2 * t, 32, stride=8), :]
            b = o_buf[p, pl.ds(2 * t + 1, 32, stride=8), :]
            even_k = (2 * p) * 512 + t * 128
            odd_k = (2 * p + 1) * 512 + t * 128
            lhs[:, even_k:even_k + 128] = jnp.where(low, a, pltpu.roll(b, 64, 1)).astype(jnp.bfloat16)
            lhs[:, odd_k:odd_k + 128] = jnp.where(low, pltpu.roll(a, 64, 1), b).astype(jnp.bfloat16)

    theirs = pl.ds(pl.multiple_of((1 - tp) * 16, 16), 16)
    mine = pl.ds(pl.multiple_of(tp * 16, 16), 16)
    tp_copies = []
    for i, (n, w) in enumerate(n_cols):
        w_copies[i].wait()
        y_buf[i, :, 0:w] = lax.dot_general(lhs[...], w_buf[n:n + w, :], (((1,), (1,)), ((), ())), preferred_element_type=jnp.float32)
        c = remote(y_buf.at[i, theirs], from_tp.at[i], tp_send.at[i], tp_recv.at[i], across_y)
        c.start()
        tp_copies.append(c)

    def rows_of(t, q):
        return pl.ds(pl.multiple_of(q * 32 + t * 16, 16), 16)

    def piece(t, q, half):
        cols = pl.ds(0, HALF) if half == 0 else pl.ds(HALF, gather.shape[1] - HALF)
        return gather.at[rows_of(t, q), cols]

    other_sp = lax.rem(sp + 2, 4)
    started = []

    def send(t, q, half, slot, peer):
        ref = piece(t, q, half)
        c = remote(ref, ref, ag_send.at[slot, half], ag_recv.at[slot, half], peer)
        c.start()
        started.append(c)

    def arrived(t, q, half, slot):
        ref = piece(t, q, half)
        remote(ref, ref, ag_send.at[slot, half], ag_recv.at[slot, half], sibling).wait_recv()

    for half in range(2):
        for i in range(3 * half, 3 * half + 3):
            n, w = n_cols[i]
            tp_copies[i].wait_recv()
            gather[rows_of(tp, sp), n:n + w] = y_buf[i, mine, 0:w] + from_tp[i, :, 0:w] + bias[0:1, n:n + w]
        send(tp, sp, half, 0, across_x)
        send(tp, sp, half, 1, across_y)
        send(tp, sp, half, 3, sibling)
    for half in range(2):
        arrived(tp, other_sp, half, 0)
        if half == 0:
            send(tp, other_sp, half, 2, across_y)
        send(tp, other_sp, half, 4, sibling)
        arrived(1 - tp, sp, half, 1)
        if half == 1:
            send(1 - tp, sp, half, 2, across_x)
        send(1 - tp, sp, half, 5, sibling)
    for half in range(2):
        arrived(1 - tp, other_sp, half, 2)
        send(1 - tp, other_sp, half, 6, sibling)
    sib = sp + 1 - 2 * core
    other_sib = lax.rem(sib + 2, 4)
    for half in range(2):
        arrived(tp, sib, half, 3)
        arrived(tp, other_sib, half, 4)
        arrived(1 - tp, sib, half, 5)
        arrived(1 - tp, other_sib, half, 6)
        lo, hi = (0, HALF) if half == 0 else (HALF, d_out)
        for n in range(lo, hi, 128):
            w = min(128, hi - n)
            y_out[n:n + w, :] = gather[:, n:n + w].T
    for c in core_copies + chip_copies + tp_copies + started:
        c.wait_send()


def exchange(part, sink_logits, w_o, b_o):
    d_out = w_o.shape[1]
    heads = w_o.shape[0]
    n_col = -(-d_out // COLS)
    padded = -(-d_out // 128) * 128
    hbm = lambda a: pltpu.with_memory_space_constraint(a, pltpu.HBM)
    vmem = pl.BlockSpec(memory_space=pltpu.VMEM)
    anyw = pl.BlockSpec(memory_space=pltpu.HBM)
    block = part.shape[1:]
    dma = pltpu.SemaphoreType.DMA
    return pl.pallas_call(
        exchange_kernel,
        out_shape=jax.ShapeDtypeStruct((d_out, 128), jnp.float32),
        in_specs=[vmem, anyw, vmem, anyw],
        out_specs=vmem,
        scratch_shapes=[
            pltpu.SMEM(sink_logits.shape, jnp.float32),
            pltpu.VMEM((d_out, heads), jnp.bfloat16),
            pltpu.VMEM((2,) + block, jnp.float32),
            pltpu.VMEM(block, jnp.float32),
            pltpu.VMEM(block, jnp.float32),
            pltpu.VMEM(block, jnp.float32),
            pltpu.VMEM((2, 256, 128), jnp.float32),
            pltpu.VMEM((32, heads), jnp.bfloat16),
            pltpu.VMEM((n_col, 32, COLS), jnp.float32),
            pltpu.VMEM((n_col, 16, COLS), jnp.float32),
            pltpu.VMEM((128, padded), jnp.float32),
            dma, dma((n_col,)), dma((2,)), dma((2,)), dma((4,)), dma((4,)), dma((n_col,)), dma((n_col,)), dma((7, 2)), dma((7, 2)),
        ],
        compiler_params=pltpu.CompilerParams(collective_id=0, has_side_effects=True, vmem_limit_bytes=32 * 1024 * 1024),
        cost_estimate=pl.CostEstimate(flops=4 * 10**8, bytes_accessed=16 * 10**6, transcendentals=10**5),
    )(part, hbm(sink_logits), b_o.astype(jnp.float32)[None, :], hbm(w_o.T))


def solution(mesh):
    cache_spec = P("dp", "sp", "tp", None)

    def block_step(hidden, seq_lens, rope_cos, rope_sin, k_cache, v_cache, norm_gain, w_qkv, b_qkv, sink_logits, w_o, b_o):
        k_out, v_out, part = local_attention(hidden, seq_lens, rope_cos, rope_sin, k_cache, v_cache, norm_gain, w_qkv, b_qkv, sink_logits)
        y_t = exchange(part, sink_logits, w_o, b_o)
        out_hidden = (hidden.T.astype(jnp.float32) + y_t).astype(jnp.bfloat16).T
        return out_hidden, k_out, v_out

    return jax.shard_map(block_step, mesh=mesh, in_specs=(P("dp", None), P("dp"), P("dp", None), P("dp", None), cache_spec, cache_spec, P(None), P(None, "tp", None), P("tp", None), P("tp"), P("tp", None), P(None)), out_specs=(P("dp", None), cache_spec, cache_spec), check_vma=False)
```

```python
import functools
import jax
import jax.numpy as jnp
from jax import lax
from jax.sharding import PartitionSpec as P
from jax.experimental import pallas as pl
from jax.experimental.pallas import tpu as pltpu

NORM_EPS = 1e-5
CHUNK = 32
GROUP = 32
PIECE = 8
AHEAD = 2
PITCH = 136
NEW = 4
PARTS = 6
MESH = pl.DeviceIdType.MESH


def attend_kernel(lens_hbm, sinks_hbm, x_hbm, gain_hbm, w_hbm, b_hbm, cos_hbm, sin_hbm, k_hbm, v_hbm,
                  k_out, v_out, part,
                  lens, sinks, todo, x_t, gain, b_qkv, cos_t, sin_t,
                  w_buf, w_f32, acc, h_buf, q_buf, kn_t, vn_t, k_buf, v_buf, e_buf,
                  small_sem, w_sem, in_sem, out_sem):
    d_model, seqs = x_t.shape
    n_chunks = seqs // CHUNK
    n_pieces = seqs // PIECE
    rows_in = d_model // PARTS

    smalls = [pltpu.make_async_copy(src, dst, small_sem.at[i]) for i, (src, dst) in enumerate(
        [(x_hbm, x_t), (gain_hbm, gain), (b_hbm, b_qkv), (cos_hbm, cos_t), (sin_hbm, sin_t), (lens_hbm, lens), (sinks_hbm, sinks)])]
    for c in smalls:
        c.start()

    def w_copy(i, c):
        rows = pl.ds(i * rows_in, rows_in)
        return pltpu.make_async_copy(w_hbm.at[rows, :, pl.ds(pl.multiple_of(c * 128, 128), 128)], w_buf.at[c, rows], w_sem.at[i, c])

    def each(n, fn):
        def step(i, carry):
            fn(i)
            return carry
        lax.fori_loop(0, n, step, 0)

    def start_w(i):
        each(5, lambda c: w_copy(i, c).start())

    each(AHEAD, start_w)

    def cache_in(a, i):
        rows = pl.ds(i * PIECE, PIECE)
        src, dst = ((k_hbm, k_buf), (v_hbm, v_buf))[a]
        return pltpu.make_async_copy(src.at[rows], dst.at[rows], in_sem.at[a, i])

    def cache_out(a, i):
        rows = pl.ds(i * PIECE, PIECE)
        src, dst = ((k_buf, k_out), (v_buf, v_out))[a]
        return pltpu.make_async_copy(src.at[rows], dst.at[rows], out_sem.at[a, i])

    for c in smalls:
        c.wait()

    base = lax.axis_index("sp") * 128

    def note(b, count):
        loc = lens[b] - base
        inside = (loc >= 0) & (loc < 128)
        todo[count] = b
        return count + jnp.where(inside, 1, 0)

    n_new = lax.fori_loop(0, seqs, note, 0)
    last = todo[jnp.maximum(n_new - 1, 0)]
    for u in range(NEW):
        todo[n_new + u] = last

    def sq_step(i, total):
        xb = x_t[pl.ds(pl.multiple_of(i * rows_in, rows_in), rows_in), :].astype(jnp.float32)
        return total + jnp.sum((xb * xb).reshape(rows_in // 8, 8, seqs), axis=0)

    sq = jnp.sum(lax.fori_loop(0, PARTS, sq_step, jnp.zeros((8, seqs), jnp.float32)), axis=0, keepdims=True)
    inv = jnp.broadcast_to(lax.rsqrt(sq * (1.0 / d_model) + NORM_EPS), (seqs, seqs)).T[:, 0:1]

    def norm_step(i):
        xb = x_t[pl.ds(pl.multiple_of(i * rows_in, rows_in), rows_in), :].astype(jnp.float32).T
        h_buf[i] = (xb * inv * gain[i]).astype(jnp.bfloat16)

    each(PARTS, norm_step)

    bias = b_qkv[...].astype(jnp.float32)
    for p in range(2):
        for c in range(5):
            for u in range(2):
                acc[p, c, :, u * 128:u * 128 + 128] = jnp.broadcast_to(bias[2 * p + u:2 * p + u + 1, c * 128:c * 128 + 128], (seqs, 128))

    def project(i):
        @pl.when(i + AHEAD < PARTS)
        def _():
            start_w(i + AHEAD)

        @pl.when(i < 2)
        def _():
            each(n_pieces // 2, lambda u: cache_in(0, i * (n_pieces // 2) + u).start())

        @pl.when((i >= 2) & (i < 4))
        def _():
            each(n_pieces // 2, lambda u: cache_in(1, (i - 2) * (n_pieces // 2) + u).start())

        each(5, lambda c: w_copy(i, c).wait())
        rows = i * rows_in

        def column(c):
            w_f32[c % 2] = w_buf[c, pl.ds(rows, rows_in)].reshape(4 * rows_in, 128).astype(jnp.float32)
            for p in range(2):
                w = jnp.concatenate([w_f32[c % 2, pl.ds(2 * p + u, rows_in, stride=4), :].astype(jnp.bfloat16) for u in range(2)], axis=1)
                acc[p, c] += jnp.dot(h_buf[i], w, preferred_element_type=jnp.float32)

        for c in range(5):
            column(c)

    each(PARTS, project)

    lane = lax.broadcasted_iota(jnp.int32, (seqs, 128), 1)
    low = lane < 64
    first_half = (lane & 63) < 32
    cos4 = jnp.concatenate([cos_t[...]] * 4, axis=0).T
    sin4 = jnp.concatenate([sin_t[...]] * 4, axis=0).T
    sin4 = jnp.where(first_half, -sin4, sin4)

    def rotate(t):
        other = jnp.where(first_half, pltpu.roll(t, 96, 1), pltpu.roll(t, 32, 1))
        return t * cos4 + other * sin4

    def halves(p, tile):
        t0 = acc[p, tile, :, 0:128]
        t1 = acc[p, tile, :, 128:256]
        return jnp.where(low, t0, pltpu.roll(t1, 64, 1)), jnp.where(low, pltpu.roll(t0, 64, 1), t1)

    for p in range(2):
        def q_step(tile):
            even, odd = halves(p, tile)
            q_buf[p, pl.ds(pl.multiple_of(2 * tile * PITCH, 8), seqs), :] = rotate(even)
            q_buf[p, pl.ds(pl.multiple_of((2 * tile + 1) * PITCH, 8), seqs), :] = rotate(odd)

        each(4, q_step)
        even, odd = halves(p, 4)
        lanes = slice(p * 128, p * 128 + 128)
        kn_t[lanes, :] = rotate(even).T.astype(jnp.bfloat16)
        vn_t[lanes, :] = odd.T.astype(jnp.bfloat16)

    lane8 = lax.broadcasted_iota(jnp.int32, (8, 128), 1)
    row8 = lax.broadcasted_iota(jnp.int32, (8, 128), 0)
    sink_rows = []
    for k in range(4):
        t = jnp.zeros((8, 128), jnp.float32)
        for g in range(8):
            t = jnp.where(row8 == g, sinks[k * 8 + g], t)
        sink_rows.append(t)
    sink_all = jnp.concatenate(sink_rows, axis=0)
    lane32 = lax.broadcasted_iota(jnp.int32, (32, 128), 1)
    lane256 = lax.broadcasted_iota(jnp.int32, (256, 128), 1)
    q_lane = lax.broadcasted_iota(jnp.int32, (8, 256), 1) // 64
    half8 = lane8 < 64

    def put_new(buf, new_t):
        def step(t, carry):
            new = []
            for u in range(NEW):
                b = todo[t * NEW + u]
                loc = lens[b] - base
                col = pltpu.roll(new_t[...], lax.rem(loc - b + 256, 128), 1)
                new.append((b, jnp.where(lane256 == loc, col, buf[b])))
            for b, tile in new:
                buf[b] = tile
            return carry

        lax.fori_loop(0, (n_new + NEW - 1) // NEW, step, 0)

    def finish(a, buf, new_t):
        each(n_pieces, lambda i: cache_in(a, i).wait())
        put_new(buf, new_t)
        each(n_pieces, lambda i: cache_out(a, i).start())

    def score_step(i, carry):
        group = i // (GROUP // CHUNK)
        m_acc = part[group, 256:264, 0:128]
        s_acc = part[group, 256:264, 128:256]
        for u in range(CHUNK):
            b = i * CHUNK + u
            j = lax.rem(i, GROUP // CHUNK) * CHUNK + u
            rows = jnp.concatenate([q_buf[p, pl.ds(b, 8, stride=PITCH), :] for p in range(2)], axis=1)
            q_blk = jnp.concatenate([jnp.where(q_lane == k, rows, 0.0) for k in range(4)], axis=0).astype(jnp.bfloat16)
            logits = jnp.dot(q_blk, k_buf[b], preferred_element_type=jnp.float32) * 0.125
            logits = jnp.where(lane32 <= lens[b] - base, logits, -jnp.inf)
            m = jnp.maximum(jnp.broadcast_to(jnp.max(logits, axis=1, keepdims=True), logits.shape), sink_all)
            e = jnp.exp(logits - m)
            s = jnp.sum(e, axis=1, keepdims=True)
            e_buf[pl.ds(pl.multiple_of(b * 32, 32), 32), :] = e.astype(jnp.bfloat16)
            for k in range(4):
                here = lane8 == j * 4 + k
                m_acc = jnp.where(here, m[8 * k:8 * k + 8], m_acc)
                s_acc = jnp.where(here, s[8 * k:8 * k + 8], s_acc)
        part[group, 256:264, 0:128] = m_acc
        part[group, 256:264, 128:256] = s_acc
        return carry

    finish(0, k_buf, kn_t)
    lax.fori_loop(0, n_chunks, score_step, 0)

    def value_step(i, carry):
        group = i // (GROUP // CHUNK)
        for u in range(CHUNK):
            b = i * CHUNK + u
            j = lax.rem(i, GROUP // CHUNK) * CHUNK + u
            e = e_buf[pl.ds(pl.multiple_of(b * 32, 32), 32), :]
            r = lax.dot_general(e, v_buf[b], (((1,), (1,)), ((), ())), preferred_element_type=jnp.float32)
            rows = pl.ds(pl.multiple_of(j * 8, 8), 8)
            part[group, rows, 0:128] = jnp.where(half8, r[0:8, 0:128], r[8:16, 0:128])
            part[group, rows, 128:256] = jnp.where(half8, r[16:24, 128:256], r[24:32, 128:256])
        return carry

    finish(1, v_buf, vn_t)
    lax.fori_loop(0, n_chunks, value_step, 0)

    def drain(i, carry):
        cache_out(0, i).wait()
        cache_out(1, i).wait()
        return carry

    lax.fori_loop(0, n_pieces, drain, 0)


def local_attention(hidden, seq_lens, rope_cos, rope_sin, k_cache, v_cache, norm_gain, w_qkv, b_qkv, sink_logits):
    seqs, d_model = hidden.shape
    ctx, kv, dim = k_cache.shape[1:]
    k_t = k_cache.transpose(0, 2, 3, 1).reshape(seqs, kv * dim, ctx)
    v_t = v_cache.transpose(0, 2, 3, 1).reshape(seqs, kv * dim, ctx)
    hbm = lambda a: pltpu.with_memory_space_constraint(a, pltpu.HBM)
    vmem = pl.BlockSpec(memory_space=pltpu.VMEM)
    anyw = pl.BlockSpec(memory_space=pltpu.HBM)
    n_chunks = seqs // PIECE
    k_out, v_out, part = pl.pallas_call(
        attend_kernel,
        out_shape=(jax.ShapeDtypeStruct(k_t.shape, k_t.dtype), jax.ShapeDtypeStruct(v_t.shape, v_t.dtype),
                   jax.ShapeDtypeStruct((seqs // GROUP, GROUP * 8 + 8, kv * dim), jnp.float32)),
        in_specs=[anyw] * 10,
        out_specs=(anyw, anyw, vmem),
        scratch_shapes=[
            pltpu.SMEM((seqs,), jnp.int32),
            pltpu.SMEM((kv * 8,), jnp.float32),
            pltpu.SMEM((seqs + NEW,), jnp.int32),
            pltpu.VMEM((d_model, seqs), jnp.bfloat16),
            pltpu.VMEM((PARTS, 1, d_model // PARTS), jnp.float32),
            pltpu.VMEM(b_qkv.shape, jnp.bfloat16),
            pltpu.VMEM((dim // 2, seqs), jnp.float32),
            pltpu.VMEM((dim // 2, seqs), jnp.float32),
            pltpu.VMEM((5, d_model, kv, 128), jnp.bfloat16),
            pltpu.VMEM((2, d_model // PARTS * kv, 128), jnp.float32),
            pltpu.VMEM((2, 5, seqs, 256), jnp.float32),
            pltpu.VMEM((PARTS, seqs, d_model // PARTS), jnp.bfloat16),
            pltpu.VMEM((2, 8 * PITCH, 128), jnp.float32),
            pltpu.VMEM((kv * dim, seqs), jnp.bfloat16),
            pltpu.VMEM((kv * dim, seqs), jnp.bfloat16),
            pltpu.VMEM(k_t.shape, jnp.bfloat16),
            pltpu.VMEM(v_t.shape, jnp.bfloat16),
            pltpu.VMEM((seqs * 32, 128), jnp.bfloat16),
            pltpu.SemaphoreType.DMA((7,)),
            pltpu.SemaphoreType.DMA((PARTS, 5)),
            pltpu.SemaphoreType.DMA((2, n_chunks)),
            pltpu.SemaphoreType.DMA((2, n_chunks)),
        ],
        compiler_params=pltpu.CompilerParams(vmem_limit_bytes=44 * 1024 * 1024),
        cost_estimate=pl.CostEstimate(flops=3 * 10**9, bytes_accessed=48 * 10**6, transcendentals=10**6),
    )(hbm(seq_lens), hbm(sink_logits), hbm(hidden.T), norm_gain.astype(jnp.float32).reshape(PARTS, 1, d_model // PARTS), hbm(w_qkv), hbm(b_qkv),
      hbm(rope_cos.T), hbm(rope_sin.T), hbm(k_t), hbm(v_t))
    back = lambda a: a.reshape(seqs, kv, dim, ctx).transpose(0, 3, 1, 2)
    return back(k_out), back(v_out), part


COLS = 512
HALF = 3 * COLS


def exchange_kernel(part, sinks_hbm, bias, w_hbm, y_out,
                    sinks, w_buf, from_core, to_chip, own, from_chip, o_buf, lhs, y_buf, from_tp, gather,
                    small_sem, w_sem, core_send, core_recv, chip_send, chip_recv, tp_send, tp_recv, ag_send, ag_recv):
    tp = lax.axis_index("tp")
    sp = lax.axis_index("sp")
    core = lax.rem(sp, 2)
    chip = sp // 2
    d_out = w_hbm.shape[0]
    n_cols = [(n, min(COLS, d_out - n)) for n in range(0, d_out, COLS)]
    sibling = {"sp": sp + 1 - 2 * core}
    across_x = {"sp": lax.rem(sp + 2, 4)}
    across_y = {"tp": 1 - tp}

    small = pltpu.make_async_copy(sinks_hbm, sinks, small_sem)
    small.start()
    w_copies = [pltpu.make_async_copy(w_hbm.at[pl.ds(n, w)], w_buf.at[pl.ds(n, w)], w_sem.at[i]) for i, (n, w) in enumerate(n_cols)]
    for c in w_copies:
        c.start()

    barrier = pltpu.get_barrier_semaphore()
    for peer in (sibling, across_x, across_y):
        pl.semaphore_signal(barrier, inc=1, device_id=peer, device_id_type=MESH)
    pl.semaphore_wait(barrier, 3)

    def remote(src, dst, ss, rs, peer):
        return pltpu.make_async_remote_copy(src_ref=src, dst_ref=dst, send_sem=ss, recv_sem=rs, device_id=peer, device_id_type=MESH)

    core_copies = []
    for r in range(2):
        x_side = (1 - chip) if r == 0 else chip
        group = 2 * x_side + (1 - core)
        core_copies.append(remote(part.at[group], from_core.at[r], core_send.at[r], core_recv.at[r], sibling))
    for c in core_copies:
        c.start()

    lane = lax.broadcasted_iota(jnp.int32, (8, 128), 1)
    row = lax.broadcasted_iota(jnp.int32, (8, 128), 0)
    high = lane // 64

    def spread(f, j, p):
        return jnp.take_along_axis(f, j * 4 + 2 * p + high, axis=1)

    def stats(a, b):
        m_a, s_a = a[0], a[1]
        m_b, s_b = b[0], b[1]
        m = jnp.maximum(m_a, m_b)
        f_a = jnp.exp(m_a - m)
        f_b = jnp.exp(m_b - m)
        return m, s_a * f_a + s_b * f_b, f_a, f_b

    def stat_rows(ref):
        return ref[256:264, 0:128], ref[256:264, 128:256]

    def merge(a_ref, b_ref, out_ref, f_a, f_b, j0, j1):
        for j in range(j0, j1):
            rows = slice(8 * j, 8 * j + 8)
            for p in range(2):
                cols = slice(128 * p, 128 * p + 128)
                out_ref[rows, cols] = a_ref[rows, cols] * spread(f_a, j, p) + b_ref[rows, cols] * spread(f_b, j, p)

    pieces = [(0, 8), (8, 16), (16, 24), (24, 32)]

    def piece_rows(i):
        j0, j1 = pieces[i]
        return pl.ds(8 * j0, 8 * (j1 - j0) + (8 if i == len(pieces) - 1 else 0))

    core_copies[0].wait_recv()
    away = part.at[2 * (1 - chip) + core]
    m, s, f_a, f_b = stats(stat_rows(away), stat_rows(from_core.at[0]))
    to_chip[256:264, 0:128] = m
    to_chip[256:264, 128:256] = s
    chip_copies = [remote(to_chip.at[piece_rows(i)], from_chip.at[piece_rows(i)], chip_send.at[i], chip_recv.at[i], across_x) for i in range(len(pieces))]
    order = [3, 0, 1, 2]
    for i in order:
        merge(away, from_core.at[0], to_chip, f_a, f_b, *pieces[i])
        chip_copies[i].start()

    core_copies[1].wait_recv()
    here = part.at[2 * chip + core]
    m_own, s_own, f_a, f_b = stats(stat_rows(here), stat_rows(from_core.at[1]))
    merge(here, from_core.at[1], own, f_a, f_b, 0, 32)

    small.wait()
    sink = jnp.zeros((8, 128), jnp.float32)
    k_of_lane = lane & 3
    for k in range(4):
        for g in range(8):
            sink = jnp.where((row == g) & (k_of_lane == k), sinks[k * 8 + g], sink)

    chip_copies[3].wait_recv()
    m, s, f_a, f_b = stats((m_own, s_own), stat_rows(from_chip))
    scale = 1.0 / (s + jnp.exp(sink - m))
    f_a = f_a * scale
    f_b = f_b * scale
    for i in order:
        if i != 3:
            chip_copies[i].wait_recv()
        for j in range(*pieces[i]):
            rows = slice(8 * j, 8 * j + 8)
            for p in range(2):
                cols = slice(128 * p, 128 * p + 128)
                o_buf[p, rows, :] = own[rows, cols] * spread(f_a, j, p) + from_chip[rows, cols] * spread(f_b, j, p)

    low = lax.broadcasted_iota(jnp.int32, (32, 128), 1) < 64
    for p in range(2):
        for t in range(4):
            a = o_buf[p, pl.ds(2 * t, 32, stride=8), :]
            b = o_buf[p, pl.ds(2 * t + 1, 32, stride=8), :]
            even_k = (2 * p) * 512 + t * 128
            odd_k = (2 * p + 1) * 512 + t * 128
            lhs[:, even_k:even_k + 128] = jnp.where(low, a, pltpu.roll(b, 64, 1)).astype(jnp.bfloat16)
            lhs[:, odd_k:odd_k + 128] = jnp.where(low, pltpu.roll(a, 64, 1), b).astype(jnp.bfloat16)

    theirs = pl.ds(pl.multiple_of((1 - tp) * 16, 16), 16)
    mine = pl.ds(pl.multiple_of(tp * 16, 16), 16)
    tp_copies = []
    for i, (n, w) in enumerate(n_cols):
        w_copies[i].wait()
        y_buf[i, :, 0:w] = lax.dot_general(lhs[...], w_buf[n:n + w, :], (((1,), (1,)), ((), ())), preferred_element_type=jnp.float32)
        c = remote(y_buf.at[i, theirs], from_tp.at[i], tp_send.at[i], tp_recv.at[i], across_y)
        c.start()
        tp_copies.append(c)

    def rows_of(t, q):
        return pl.ds(pl.multiple_of(q * 32 + t * 16, 16), 16)

    def piece(t, q, half):
        cols = pl.ds(0, HALF) if half == 0 else pl.ds(HALF, gather.shape[1] - HALF)
        return gather.at[rows_of(t, q), cols]

    other_sp = lax.rem(sp + 2, 4)
    started = []

    def send(t, q, half, slot, peer):
        ref = piece(t, q, half)
        c = remote(ref, ref, ag_send.at[slot, half], ag_recv.at[slot, half], peer)
        c.start()
        started.append(c)

    def arrived(t, q, half, slot):
        ref = piece(t, q, half)
        remote(ref, ref, ag_send.at[slot, half], ag_recv.at[slot, half], sibling).wait_recv()

    for half in range(2):
        for i in range(3 * half, 3 * half + 3):
            n, w = n_cols[i]
            tp_copies[i].wait_recv()
            gather[rows_of(tp, sp), n:n + w] = y_buf[i, mine, 0:w] + from_tp[i, :, 0:w] + bias[0:1, n:n + w]
        send(tp, sp, half, 0, across_x)
        send(tp, sp, half, 1, across_y)
        send(tp, sp, half, 3, sibling)
    for half in range(2):
        arrived(tp, other_sp, half, 0)
        if half == 0:
            send(tp, other_sp, half, 2, across_y)
        send(tp, other_sp, half, 4, sibling)
        arrived(1 - tp, sp, half, 1)
        if half == 1:
            send(1 - tp, sp, half, 2, across_x)
        send(1 - tp, sp, half, 5, sibling)
    for half in range(2):
        arrived(1 - tp, other_sp, half, 2)
        send(1 - tp, other_sp, half, 6, sibling)
    sib = sp + 1 - 2 * core
    other_sib = lax.rem(sib + 2, 4)
    for half in range(2):
        arrived(tp, sib, half, 3)
        arrived(tp, other_sib, half, 4)
        arrived(1 - tp, sib, half, 5)
        arrived(1 - tp, other_sib, half, 6)
        lo, hi = (0, HALF) if half == 0 else (HALF, d_out)
        for n in range(lo, hi, 128):
            w = min(128, hi - n)
            y_out[n:n + w, :] = gather[:, n:n + w].T
    for c in core_copies + chip_copies + tp_copies + started:
        c.wait_send()


def exchange(part, sink_logits, w_o, b_o):
    d_out = w_o.shape[1]
    heads = w_o.shape[0]
    n_col = -(-d_out // COLS)
    padded = -(-d_out // 128) * 128
    hbm = lambda a: pltpu.with_memory_space_constraint(a, pltpu.HBM)
    vmem = pl.BlockSpec(memory_space=pltpu.VMEM)
    anyw = pl.BlockSpec(memory_space=pltpu.HBM)
    block = part.shape[1:]
    dma = pltpu.SemaphoreType.DMA
    return pl.pallas_call(
        exchange_kernel,
        out_shape=jax.ShapeDtypeStruct((d_out, 128), jnp.float32),
        in_specs=[vmem, anyw, vmem, anyw],
        out_specs=vmem,
        scratch_shapes=[
            pltpu.SMEM(sink_logits.shape, jnp.float32),
            pltpu.VMEM((d_out, heads), jnp.bfloat16),
            pltpu.VMEM((2,) + block, jnp.float32),
            pltpu.VMEM(block, jnp.float32),
            pltpu.VMEM(block, jnp.float32),
            pltpu.VMEM(block, jnp.float32),
            pltpu.VMEM((2, 256, 128), jnp.float32),
            pltpu.VMEM((32, heads), jnp.bfloat16),
            pltpu.VMEM((n_col, 32, COLS), jnp.float32),
            pltpu.VMEM((n_col, 16, COLS), jnp.float32),
            pltpu.VMEM((128, padded), jnp.float32),
            dma, dma((n_col,)), dma((2,)), dma((2,)), dma((4,)), dma((4,)), dma((n_col,)), dma((n_col,)), dma((7, 2)), dma((7, 2)),
        ],
        compiler_params=pltpu.CompilerParams(collective_id=0, has_side_effects=True, vmem_limit_bytes=32 * 1024 * 1024),
        cost_estimate=pl.CostEstimate(flops=4 * 10**8, bytes_accessed=16 * 10**6, transcendentals=10**5),
    )(part, hbm(sink_logits), b_o.astype(jnp.float32)[None, :], hbm(w_o.T))


def solution(mesh):
    cache_spec = P("dp", "sp", "tp", None)

    def block_step(hidden, seq_lens, rope_cos, rope_sin, k_cache, v_cache, norm_gain, w_qkv, b_qkv, sink_logits, w_o, b_o):
        k_out, v_out, part = local_attention(hidden, seq_lens, rope_cos, rope_sin, k_cache, v_cache, norm_gain, w_qkv, b_qkv, sink_logits)
        y_t = exchange(part, sink_logits, w_o, b_o)
        out_hidden = (hidden.T.astype(jnp.float32) + y_t).astype(jnp.bfloat16).T
        return out_hidden, k_out, v_out

    return jax.shard_map(block_step, mesh=mesh, in_specs=(P("dp", None), P("dp"), P("dp", None), P("dp", None), cache_spec, cache_spec, P(None), P(None, "tp", None), P("tp", None), P("tp"), P("tp", None), P(None)), out_specs=(P("dp", None), cache_spec, cache_spec), check_vma=False)
```

```python
import functools
import jax
import jax.numpy as jnp
from jax import lax
from jax.sharding import PartitionSpec as P
from jax.experimental import pallas as pl
from jax.experimental.pallas import tpu as pltpu

NORM_EPS = 1e-5
GROUP = 32
PIECE = 16
AHEAD = 3
PITCH = 136
NEW = 4
PARTS = 6
MESH = pl.DeviceIdType.MESH


def each(n, fn):
    def step(i, carry):
        fn(i)
        return carry
    lax.fori_loop(0, n, step, 0)


def sink_table(sinks):
    row = lax.broadcasted_iota(jnp.int32, (8, 128), 0)
    rows = []
    for k in range(4):
        t = jnp.zeros((8, 128), jnp.float32)
        for g in range(8):
            t = jnp.where(row == g, sinks[k * 8 + g], t)
        rows.append(t)
    return rows


def score_group(first, base, lens, sink_all, q_buf, keys, e_buf, out):
    lane8 = lax.broadcasted_iota(jnp.int32, (8, 128), 1)
    lane32 = lax.broadcasted_iota(jnp.int32, (32, 128), 1)
    q_lane = lax.broadcasted_iota(jnp.int32, (8, 256), 1) // 64
    m_acc = jnp.zeros((8, 128), jnp.float32)
    s_acc = jnp.zeros((8, 128), jnp.float32)
    for u in range(GROUP):
        b = first + u
        rows = jnp.concatenate([q_buf[p, pl.ds(b, 8, stride=PITCH), :] for p in range(2)], axis=1)
        q_blk = jnp.concatenate([jnp.where(q_lane == k, rows, 0.0) for k in range(4)], axis=0).astype(jnp.bfloat16)
        logits = jnp.dot(q_blk, keys(u), preferred_element_type=jnp.float32) * 0.125
        logits = jnp.where(lane32 <= lens[b] - base, logits, -jnp.inf)
        m = jnp.maximum(jnp.broadcast_to(jnp.max(logits, axis=1, keepdims=True), logits.shape), sink_all)
        e = jnp.exp(logits - m)
        s = jnp.sum(e, axis=1, keepdims=True)
        e_buf[32 * u:32 * u + 32, :] = e.astype(jnp.bfloat16)
        for k in range(4):
            here = lane8 == u * 4 + k
            m_acc = jnp.where(here, m[8 * k:8 * k + 8], m_acc)
            s_acc = jnp.where(here, s[8 * k:8 * k + 8], s_acc)
    out[256:264, 0:128] = m_acc
    out[256:264, 128:256] = s_acc


def value_group(values, e_buf, out):
    half8 = lax.broadcasted_iota(jnp.int32, (8, 128), 1) < 64
    for u in range(GROUP):
        r = lax.dot_general(e_buf[32 * u:32 * u + 32, :], values(u), (((1,), (1,)), ((), ())), preferred_element_type=jnp.float32)
        out[8 * u:8 * u + 8, 0:128] = jnp.where(half8, r[0:8, 0:128], r[8:16, 0:128])
        out[8 * u:8 * u + 8, 128:256] = jnp.where(half8, r[16:24, 128:256], r[24:32, 128:256])


def attend_kernel(lens_hbm, sinks_hbm, x_hbm, gain_hbm, w_hbm, b_hbm, cos_hbm, sin_hbm, k_hbm, v_hbm,
                  k_out, v_out, part, q_buf,
                  lens, sinks, todo, x_t, gain, b_qkv, cos_t, sin_t,
                  w_buf, w_f32, acc, h_buf, kn_t, vn_t, k_buf, v_buf, e_buf,
                  small_sem, w_sem, in_sem, out_sem):
    d_model, seqs = x_t.shape
    n_pieces = seqs // PIECE
    rows_in = d_model // PARTS

    smalls = [pltpu.make_async_copy(src, dst, small_sem.at[i]) for i, (src, dst) in enumerate(
        [(x_hbm, x_t), (gain_hbm, gain), (b_hbm, b_qkv), (cos_hbm, cos_t), (sin_hbm, sin_t), (lens_hbm, lens), (sinks_hbm, sinks)])]
    for c in smalls:
        c.start()

    def w_copy(i, c):
        rows = pl.ds(i * rows_in, rows_in)
        return pltpu.make_async_copy(w_hbm.at[rows, :, pl.ds(pl.multiple_of(c * 128, 128), 128)], w_buf.at[c, rows], w_sem.at[i, c])

    def start_w(i):
        each(5, lambda c: w_copy(i, c).start())

    each(AHEAD, start_w)

    def cache_in(a, i):
        rows = pl.ds(i * PIECE, PIECE)
        src, dst = ((k_hbm, k_buf), (v_hbm, v_buf))[a]
        return pltpu.make_async_copy(src.at[rows], dst.at[rows], in_sem.at[a, i])

    def cache_out(a, i):
        rows = pl.ds(i * PIECE, PIECE)
        src, dst = ((k_buf, k_out), (v_buf, v_out))[a]
        return pltpu.make_async_copy(src.at[rows], dst.at[rows], out_sem.at[a, i])

    for c in smalls:
        c.wait()

    base = lax.axis_index("sp") * 128

    def note(b, count):
        loc = lens[b] - base
        inside = (loc >= 0) & (loc < 128)
        todo[count] = b
        return count + jnp.where(inside, 1, 0)

    n_new = lax.fori_loop(0, seqs, note, 0)
    last = todo[jnp.maximum(n_new - 1, 0)]
    for u in range(NEW):
        todo[n_new + u] = last

    def sq_step(i, total):
        xb = x_t[pl.ds(pl.multiple_of(i * rows_in, rows_in), rows_in), :].astype(jnp.float32)
        return total + jnp.sum((xb * xb).reshape(rows_in // 8, 8, seqs), axis=0)

    sq = jnp.sum(lax.fori_loop(0, PARTS, sq_step, jnp.zeros((8, seqs), jnp.float32)), axis=0, keepdims=True)
    inv = jnp.broadcast_to(lax.rsqrt(sq * (1.0 / d_model) + NORM_EPS), (seqs, seqs)).T[:, 0:1]

    def norm_step(i):
        xb = x_t[pl.ds(pl.multiple_of(i * rows_in, rows_in), rows_in), :].astype(jnp.float32).T
        h_buf[i] = (xb * inv * gain[i]).astype(jnp.bfloat16)

    each(PARTS, norm_step)

    bias = b_qkv[...].astype(jnp.float32)
    for p in range(2):
        for c in range(5):
            for u in range(2):
                acc[p, c, :, u * 128:u * 128 + 128] = jnp.broadcast_to(bias[2 * p + u:2 * p + u + 1, c * 128:c * 128 + 128], (seqs, 128))

    def project(i):
        @pl.when(i + AHEAD < PARTS)
        def _():
            start_w(i + AHEAD)

        @pl.when(i < 2)
        def _():
            each(n_pieces // 2, lambda u: cache_in(0, i * (n_pieces // 2) + u).start())

        @pl.when((i >= 2) & (i < 4))
        def _():
            each(n_pieces // 2, lambda u: cache_in(1, (i - 2) * (n_pieces // 2) + u).start())

        each(5, lambda c: w_copy(i, c).wait())
        rows = i * rows_in

        def column(c):
            w_f32[c % 2] = w_buf[c, pl.ds(rows, rows_in)].reshape(4 * rows_in, 128).astype(jnp.float32)
            for p in range(2):
                w = jnp.concatenate([w_f32[c % 2, pl.ds(2 * p + u, rows_in, stride=4), :].astype(jnp.bfloat16) for u in range(2)], axis=1)
                acc[p, c] += jnp.dot(h_buf[i], w, preferred_element_type=jnp.float32)

        for c in range(5):
            column(c)

    each(PARTS, project)

    lane = lax.broadcasted_iota(jnp.int32, (seqs, 128), 1)
    low = lane < 64
    first_half = (lane & 63) < 32
    cos4 = jnp.concatenate([cos_t[...]] * 4, axis=0).T
    sin4 = jnp.concatenate([sin_t[...]] * 4, axis=0).T
    sin4 = jnp.where(first_half, -sin4, sin4)

    def rotate(t):
        other = jnp.where(first_half, pltpu.roll(t, 96, 1), pltpu.roll(t, 32, 1))
        return t * cos4 + other * sin4

    def halves(p, tile):
        t0 = acc[p, tile, :, 0:128]
        t1 = acc[p, tile, :, 128:256]
        return jnp.where(low, t0, pltpu.roll(t1, 64, 1)), jnp.where(low, pltpu.roll(t0, 64, 1), t1)

    for p in range(2):
        def q_step(tile):
            even, odd = halves(p, tile)
            q_buf[p, pl.ds(pl.multiple_of(2 * tile * PITCH, 8), seqs), :] = rotate(even)
            q_buf[p, pl.ds(pl.multiple_of((2 * tile + 1) * PITCH, 8), seqs), :] = rotate(odd)

        each(4, q_step)
        even, odd = halves(p, 4)
        lanes = slice(p * 128, p * 128 + 128)
        kn_t[lanes, :] = rotate(even).T.astype(jnp.bfloat16)
        vn_t[lanes, :] = odd.T.astype(jnp.bfloat16)

    sink_all = jnp.concatenate(sink_table(sinks), axis=0)
    lane256 = lax.broadcasted_iota(jnp.int32, (256, 128), 1)
    def put_new(buf, new_t):
        def step(t, carry):
            new = []
            for u in range(NEW):
                b = todo[t * NEW + u]
                loc = lens[b] - base
                col = pltpu.roll(new_t[...], lax.rem(loc - b + 256, 128), 1)
                new.append((b, jnp.where(lane256 == loc, col, buf[b])))
            for b, tile in new:
                buf[b] = tile
            return carry

        lax.fori_loop(0, (n_new + NEW - 1) // NEW, step, 0)

    def finish(a, buf, new_t):
        each(n_pieces, lambda i: cache_in(a, i).wait())
        put_new(buf, new_t)
        each(n_pieces, lambda i: cache_out(a, i).start())

    away = (1 - lax.axis_index("sp") // 2) * 2 * GROUP
    finish(0, k_buf, kn_t)

    def score_away(t):
        first = away + t * GROUP
        score_group(first, base, lens, sink_all, q_buf, lambda u: k_buf[first + u], e_buf.at[t], part.at[t])

    each(2, score_away)
    finish(1, v_buf, vn_t)

    def value_away(t):
        first = away + t * GROUP
        value_group(lambda u: v_buf[first + u], e_buf.at[t], part.at[t])

    each(2, value_away)

    def drain(i, carry):
        cache_out(0, i).wait()
        cache_out(1, i).wait()
        return carry

    lax.fori_loop(0, n_pieces, drain, 0)


def local_attention(hidden, seq_lens, rope_cos, rope_sin, k_cache, v_cache, norm_gain, w_qkv, b_qkv, sink_logits):
    seqs, d_model = hidden.shape
    ctx, kv, dim = k_cache.shape[1:]
    k_t = k_cache.transpose(0, 2, 3, 1).reshape(seqs, kv * dim, ctx)
    v_t = v_cache.transpose(0, 2, 3, 1).reshape(seqs, kv * dim, ctx)
    hbm = lambda a: pltpu.with_memory_space_constraint(a, pltpu.HBM)
    vmem = pl.BlockSpec(memory_space=pltpu.VMEM)
    anyw = pl.BlockSpec(memory_space=pltpu.HBM)
    n_chunks = seqs // PIECE
    k_out, v_out, part, q_buf = pl.pallas_call(
        attend_kernel,
        out_shape=(jax.ShapeDtypeStruct(k_t.shape, k_t.dtype), jax.ShapeDtypeStruct(v_t.shape, v_t.dtype),
                   jax.ShapeDtypeStruct((2, GROUP * 8 + 8, kv * dim), jnp.float32),
                   jax.ShapeDtypeStruct((2, 8 * PITCH, 128), jnp.float32)),
        in_specs=[anyw] * 10,
        out_specs=(anyw, anyw, vmem, vmem),
        scratch_shapes=[
            pltpu.SMEM((seqs,), jnp.int32),
            pltpu.SMEM((kv * 8,), jnp.float32),
            pltpu.SMEM((seqs + NEW,), jnp.int32),
            pltpu.VMEM((d_model, seqs), jnp.bfloat16),
            pltpu.VMEM((PARTS, 1, d_model // PARTS), jnp.float32),
            pltpu.VMEM(b_qkv.shape, jnp.bfloat16),
            pltpu.VMEM((dim // 2, seqs), jnp.float32),
            pltpu.VMEM((dim // 2, seqs), jnp.float32),
            pltpu.VMEM((5, d_model, kv, 128), jnp.bfloat16),
            pltpu.VMEM((2, d_model // PARTS * kv, 128), jnp.float32),
            pltpu.VMEM((2, 5, seqs, 256), jnp.float32),
            pltpu.VMEM((PARTS, seqs, d_model // PARTS), jnp.bfloat16),
            pltpu.VMEM((kv * dim, seqs), jnp.bfloat16),
            pltpu.VMEM((kv * dim, seqs), jnp.bfloat16),
            pltpu.VMEM(k_t.shape, jnp.bfloat16),
            pltpu.VMEM(v_t.shape, jnp.bfloat16),
            pltpu.VMEM((2, GROUP * 32, 128), jnp.bfloat16),
            pltpu.SemaphoreType.DMA((7,)),
            pltpu.SemaphoreType.DMA((PARTS, 5)),
            pltpu.SemaphoreType.DMA((2, n_chunks)),
            pltpu.SemaphoreType.DMA((2, n_chunks)),
        ],
        compiler_params=pltpu.CompilerParams(vmem_limit_bytes=44 * 1024 * 1024),
        cost_estimate=pl.CostEstimate(flops=3 * 10**9, bytes_accessed=48 * 10**6, transcendentals=10**6),
    )(hbm(seq_lens), hbm(sink_logits), hbm(hidden.T), norm_gain.astype(jnp.float32).reshape(PARTS, 1, d_model // PARTS), hbm(w_qkv), hbm(b_qkv),
      hbm(rope_cos.T), hbm(rope_sin.T), hbm(k_t), hbm(v_t))
    return k_out, v_out, part, q_buf


COLS = 512
HALF = 3 * COLS


def exchange_kernel(part, q_buf, k_hbm, v_hbm, lens_hbm, sinks_hbm, bias, w_hbm, y_out,
                    lens, sinks, k_buf, v_buf, e_buf, mine_part, w_buf, from_core, to_chip, own, from_chip, o_buf, lhs, y_buf, from_tp, gather,
                    small_sem, kv_sem, w_sem, core_send, core_recv, chip_send, chip_recv, tp_send, tp_recv, ag_send, ag_recv):
    tp = lax.axis_index("tp")
    sp = lax.axis_index("sp")
    core = lax.rem(sp, 2)
    chip = sp // 2
    d_out = w_hbm.shape[0]
    n_cols = [(n, min(COLS, d_out - n)) for n in range(0, d_out, COLS)]
    sibling = {"sp": sp + 1 - 2 * core}
    across_x = {"sp": lax.rem(sp + 2, 4)}
    across_y = {"tp": 1 - tp}

    smalls = [pltpu.make_async_copy(sinks_hbm, sinks, small_sem.at[0]), pltpu.make_async_copy(lens_hbm, lens, small_sem.at[1])]
    first_own = pl.multiple_of(chip * 2 * GROUP, GROUP)
    kv_copies = [[pltpu.make_async_copy(src.at[pl.ds(first_own + t * GROUP, GROUP)], dst.at[pl.ds(t * GROUP, GROUP)], kv_sem.at[a, t]) for t in range(2)]
                 for a, (src, dst) in enumerate(((k_hbm, k_buf), (v_hbm, v_buf)))]
    for c in smalls + kv_copies[0] + kv_copies[1]:
        c.start()
    w_copies = [pltpu.make_async_copy(w_hbm.at[pl.ds(n, w)], w_buf.at[pl.ds(n, w)], w_sem.at[i]) for i, (n, w) in enumerate(n_cols)]
    for c in w_copies:
        c.start()

    barrier = pltpu.get_barrier_semaphore()
    for peer in (sibling, across_x, across_y):
        pl.semaphore_signal(barrier, inc=1, device_id=peer, device_id_type=MESH)
    pl.semaphore_wait(barrier, 3)

    def remote(src, dst, ss, rs, peer):
        return pltpu.make_async_remote_copy(src_ref=src, dst_ref=dst, send_sem=ss, recv_sem=rs, device_id=peer, device_id_type=MESH)

    pieces = [(0, 8), (8, 16), (16, 24), (24, 32)]
    order = [3, 0, 1, 2]

    def piece_rows(i):
        j0, j1 = pieces[i]
        return pl.ds(8 * j0, 8 * (j1 - j0) + (8 if i == len(pieces) - 1 else 0))

    away_theirs = part.at[1 - core]
    core_copies = [remote(away_theirs.at[piece_rows(i)], from_core.at[0, piece_rows(i)], core_send.at[i], core_recv.at[i], sibling) for i in range(4)]
    for i in order:
        core_copies[i].start()

    lane = lax.broadcasted_iota(jnp.int32, (8, 128), 1)
    high = lane // 64

    def spread(f, j, p):
        return jnp.take_along_axis(f, j * 4 + 2 * p + high, axis=1)

    def stats(a, b):
        m_a, s_a = a[0], a[1]
        m_b, s_b = b[0], b[1]
        m = jnp.maximum(m_a, m_b)
        f_a = jnp.exp(m_a - m)
        f_b = jnp.exp(m_b - m)
        return m, s_a * f_a + s_b * f_b, f_a, f_b

    def stat_rows(ref):
        return ref[256:264, 0:128], ref[256:264, 128:256]

    def merge(a_ref, b_ref, out_ref, f_a, f_b, j0, j1):
        for j in range(j0, j1):
            rows = slice(8 * j, 8 * j + 8)
            for p in range(2):
                cols = slice(128 * p, 128 * p + 128)
                out_ref[rows, cols] = a_ref[rows, cols] * spread(f_a, j, p) + b_ref[rows, cols] * spread(f_b, j, p)

    core_copies[3].wait_recv()
    away = part.at[core]
    m, s, f_a, f_b = stats(stat_rows(away), stat_rows(from_core.at[0]))
    to_chip[256:264, 0:128] = m
    to_chip[256:264, 128:256] = s
    chip_copies = [remote(to_chip.at[piece_rows(i)], from_chip.at[piece_rows(i)], chip_send.at[i], chip_recv.at[i], across_x) for i in range(len(pieces))]
    for i in order:
        if i != 3:
            core_copies[i].wait_recv()
        merge(away, from_core.at[0], to_chip, f_a, f_b, *pieces[i])
        chip_copies[i].start()

    for c in smalls:
        c.wait()
    base = sp * 128
    sink_rows = sink_table(sinks)
    sink_all = jnp.concatenate(sink_rows, axis=0)
    for c in kv_copies[0]:
        c.wait()
    each(2, lambda t: score_group(first_own + t * GROUP, base, lens, sink_all, q_buf, lambda u: k_buf[t * GROUP + u], e_buf.at[t], mine_part.at[t]))
    for c in kv_copies[1]:
        c.wait()
    each(2, lambda t: value_group(lambda u: v_buf[t * GROUP + u], e_buf.at[t], mine_part.at[t]))
    core_copies.append(remote(mine_part.at[1 - core], from_core.at[1], core_send.at[4], core_recv.at[4], sibling))
    core_copies[4].start()

    sink = sink_rows[3]
    for k in range(3):
        sink = jnp.where((lane & 3) == k, sink_rows[k], sink)

    core_copies[4].wait_recv()
    here = mine_part.at[core]
    m_own, s_own, f_a, f_b = stats(stat_rows(here), stat_rows(from_core.at[1]))
    merge(here, from_core.at[1], own, f_a, f_b, 0, 32)

    chip_copies[3].wait_recv()
    m, s, f_a, f_b = stats((m_own, s_own), stat_rows(from_chip))
    scale = 1.0 / (s + jnp.exp(sink - m))
    f_a = f_a * scale
    f_b = f_b * scale
    for i in order:
        if i != 3:
            chip_copies[i].wait_recv()
        for j in range(*pieces[i]):
            rows = slice(8 * j, 8 * j + 8)
            for p in range(2):
                cols = slice(128 * p, 128 * p + 128)
                o_buf[p, rows, :] = own[rows, cols] * spread(f_a, j, p) + from_chip[rows, cols] * spread(f_b, j, p)

    low = lax.broadcasted_iota(jnp.int32, (32, 128), 1) < 64
    for p in range(2):
        for t in range(4):
            a = o_buf[p, pl.ds(2 * t, 32, stride=8), :]
            b = o_buf[p, pl.ds(2 * t + 1, 32, stride=8), :]
            even_k = (2 * p) * 512 + t * 128
            odd_k = (2 * p + 1) * 512 + t * 128
            lhs[:, even_k:even_k + 128] = jnp.where(low, a, pltpu.roll(b, 64, 1)).astype(jnp.bfloat16)
            lhs[:, odd_k:odd_k + 128] = jnp.where(low, pltpu.roll(a, 64, 1), b).astype(jnp.bfloat16)

    theirs = pl.ds(pl.multiple_of((1 - tp) * 16, 16), 16)
    mine = pl.ds(pl.multiple_of(tp * 16, 16), 16)
    tp_copies = []
    for i, (n, w) in enumerate(n_cols):
        w_copies[i].wait()
        y_buf[i, :, 0:w] = lax.dot_general(lhs[...], w_buf[n:n + w, :], (((1,), (1,)), ((), ())), preferred_element_type=jnp.float32)
        c = remote(y_buf.at[i, theirs], from_tp.at[i], tp_send.at[i], tp_recv.at[i], across_y)
        c.start()
        tp_copies.append(c)

    def rows_of(t, q):
        return pl.ds(pl.multiple_of(q * 32 + t * 16, 16), 16)

    def piece(t, q, half):
        cols = pl.ds(0, HALF) if half == 0 else pl.ds(HALF, gather.shape[1] - HALF)
        return gather.at[rows_of(t, q), cols]

    other_sp = lax.rem(sp + 2, 4)
    started = []

    def send(t, q, half, slot, peer):
        ref = piece(t, q, half)
        c = remote(ref, ref, ag_send.at[slot, half], ag_recv.at[slot, half], peer)
        c.start()
        started.append(c)

    def arrived(t, q, half, slot):
        ref = piece(t, q, half)
        remote(ref, ref, ag_send.at[slot, half], ag_recv.at[slot, half], sibling).wait_recv()

    for half in range(2):
        for i in range(3 * half, 3 * half + 3):
            n, w = n_cols[i]
            tp_copies[i].wait_recv()
            gather[rows_of(tp, sp), n:n + w] = y_buf[i, mine, 0:w] + from_tp[i, :, 0:w] + bias[0:1, n:n + w]
        send(tp, sp, half, 0, across_x)
        send(tp, sp, half, 1, across_y)
        send(tp, sp, half, 3, sibling)
    for half in range(2):
        arrived(tp, other_sp, half, 0)
        if half == 0:
            send(tp, other_sp, half, 2, across_y)
        send(tp, other_sp, half, 4, sibling)
        arrived(1 - tp, sp, half, 1)
        if half == 1:
            send(1 - tp, sp, half, 2, across_x)
        send(1 - tp, sp, half, 5, sibling)
    for half in range(2):
        arrived(1 - tp, other_sp, half, 2)
        send(1 - tp, other_sp, half, 6, sibling)
    sib = sp + 1 - 2 * core
    other_sib = lax.rem(sib + 2, 4)
    for half in range(2):
        arrived(tp, sib, half, 3)
        arrived(tp, other_sib, half, 4)
        arrived(1 - tp, sib, half, 5)
        arrived(1 - tp, other_sib, half, 6)
        lo, hi = (0, HALF) if half == 0 else (HALF, d_out)
        for n in range(lo, hi, 128):
            w = min(128, hi - n)
            y_out[n:n + w, :] = gather[:, n:n + w].T
    for c in core_copies + chip_copies + tp_copies + started:
        c.wait_send()


def exchange(part, q_buf, k_out, v_out, seq_lens, sink_logits, w_o, b_o):
    d_out = w_o.shape[1]
    heads = w_o.shape[0]
    n_col = -(-d_out // COLS)
    padded = -(-d_out // 128) * 128
    hbm = lambda a: pltpu.with_memory_space_constraint(a, pltpu.HBM)
    vmem = pl.BlockSpec(memory_space=pltpu.VMEM)
    anyw = pl.BlockSpec(memory_space=pltpu.HBM)
    block = part.shape[1:]
    dma = pltpu.SemaphoreType.DMA
    return pl.pallas_call(
        exchange_kernel,
        out_shape=jax.ShapeDtypeStruct((d_out, 128), jnp.float32),
        in_specs=[vmem, vmem, anyw, anyw, anyw, anyw, vmem, anyw],
        out_specs=vmem,
        scratch_shapes=[
            pltpu.SMEM(seq_lens.shape, jnp.int32),
            pltpu.SMEM(sink_logits.shape, jnp.float32),
            pltpu.VMEM((2 * GROUP,) + k_out.shape[1:], jnp.bfloat16),
            pltpu.VMEM((2 * GROUP,) + k_out.shape[1:], jnp.bfloat16),
            pltpu.VMEM((2, GROUP * 32, 128), jnp.bfloat16),
            pltpu.VMEM((2,) + block, jnp.float32),
            pltpu.VMEM((d_out, heads), jnp.bfloat16),
            pltpu.VMEM((2,) + block, jnp.float32),
            pltpu.VMEM(block, jnp.float32),
            pltpu.VMEM(block, jnp.float32),
            pltpu.VMEM(block, jnp.float32),
            pltpu.VMEM((2, 256, 128), jnp.float32),
            pltpu.VMEM((32, heads), jnp.bfloat16),
            pltpu.VMEM((n_col, 32, COLS), jnp.float32),
            pltpu.VMEM((n_col, 16, COLS), jnp.float32),
            pltpu.VMEM((128, padded), jnp.float32),
            dma((2,)), dma((2, 2)), dma((n_col,)), dma((5,)), dma((5,)), dma((4,)), dma((4,)), dma((n_col,)), dma((n_col,)), dma((7, 2)), dma((7, 2)),
        ],
        compiler_params=pltpu.CompilerParams(collective_id=0, has_side_effects=True, vmem_limit_bytes=40 * 1024 * 1024),
        cost_estimate=pl.CostEstimate(flops=4 * 10**8, bytes_accessed=16 * 10**6, transcendentals=10**5),
      )(part, q_buf, hbm(k_out), hbm(v_out), hbm(seq_lens), hbm(sink_logits), b_o.astype(jnp.float32)[None, :], hbm(w_o.T))


def solution(mesh):
    cache_spec = P("dp", "sp", "tp", None)

    def block_step(hidden, seq_lens, rope_cos, rope_sin, k_cache, v_cache, norm_gain, w_qkv, b_qkv, sink_logits, w_o, b_o):
        k_out, v_out, part, q_buf = local_attention(hidden, seq_lens, rope_cos, rope_sin, k_cache, v_cache, norm_gain, w_qkv, b_qkv, sink_logits)
        y_t = exchange(part, q_buf, k_out, v_out, seq_lens, sink_logits, w_o, b_o)
        out_hidden = (hidden.T.astype(jnp.float32) + y_t).astype(jnp.bfloat16).T
        seqs, ctx, kv, dim = k_cache.shape
        back = lambda a: a.reshape(seqs, kv, dim, ctx).transpose(0, 3, 1, 2)
        return out_hidden, back(k_out), back(v_out)

    return jax.shard_map(block_step, mesh=mesh, in_specs=(P("dp", None), P("dp"), P("dp", None), P("dp", None), cache_spec, cache_spec, P(None), P(None, "tp", None), P("tp", None), P("tp"), P("tp", None), P(None)), out_specs=(P("dp", None), cache_spec, cache_spec), check_vma=False)
```

```python
import functools
import jax
import jax.numpy as jnp
from jax import lax
from jax.sharding import PartitionSpec as P
from jax.experimental import pallas as pl
from jax.experimental.pallas import tpu as pltpu

NORM_EPS = 1e-5
GROUP = 32
LANES = 128
LO = slice(0, LANES)
HI = slice(LANES, 2 * LANES)
STAT = slice(8 * GROUP, 8 * GROUP + 8)
PIECE = 32
AHEAD = 3
PITCH = 136
NEW = 8
PARTS = 6
BLOCKS = 6
MESH = pl.DeviceIdType.MESH


def each(n, fn):
    def step(i, carry):
        fn(i)
        return carry
    lax.fori_loop(0, n, step, 0)


def sink_table(sinks):
    row = lax.broadcasted_iota(jnp.int32, (8, 128), 0)
    rows = []
    for k in range(4):
        t = jnp.zeros((8, 128), jnp.float32)
        for g in range(8):
            t = jnp.where(row == g, sinks[k * 8 + g], t)
        rows.append(t)
    return rows


def score_group(first, base, lens, sink_all, q_buf, keys, e_buf, out):
    lane8 = lax.broadcasted_iota(jnp.int32, (8, 128), 1)
    lane32 = lax.broadcasted_iota(jnp.int32, (32, 128), 1)
    q_lane = lax.broadcasted_iota(jnp.int32, (8, 256), 1) // 64
    m_acc = jnp.zeros((8, 128), jnp.float32)
    s_acc = jnp.zeros((8, 128), jnp.float32)
    for u in range(GROUP):
        b = first + u
        rows = jnp.concatenate([q_buf[p, pl.ds(b, 8, stride=PITCH), :] for p in range(2)], axis=1)
        q_blk = jnp.concatenate([jnp.where(q_lane == k, rows, 0.0) for k in range(4)], axis=0).astype(jnp.bfloat16)
        logits = jnp.dot(q_blk, keys(u), preferred_element_type=jnp.float32) * 0.125
        logits = jnp.where(lane32 <= lens[b] - base, logits, -jnp.inf)
        m = jnp.maximum(jnp.broadcast_to(jnp.max(logits, axis=1, keepdims=True), logits.shape), sink_all)
        e = jnp.exp(logits - m)
        s = jnp.sum(e, axis=1, keepdims=True)
        e_buf[32 * u:32 * u + 32, :] = e.astype(jnp.bfloat16)
        for k in range(4):
            here = lane8 == u * 4 + k
            m_acc = jnp.where(here, m[8 * k:8 * k + 8], m_acc)
            s_acc = jnp.where(here, s[8 * k:8 * k + 8], s_acc)
    out[STAT, LO] = m_acc
    out[STAT, HI] = s_acc


def value_group(values, e_buf, out):
    half8 = lax.broadcasted_iota(jnp.int32, (8, 128), 1) < 64
    for u in range(GROUP):
        r = lax.dot_general(e_buf[32 * u:32 * u + 32, :], values(u), (((1,), (1,)), ((), ())), preferred_element_type=jnp.float32)
        out[8 * u:8 * u + 8, LO] = jnp.where(half8, r[0:8, LO], r[8:16, LO])
        out[8 * u:8 * u + 8, HI] = jnp.where(half8, r[16:24, HI], r[24:32, HI])


def attend_kernel(lens_hbm, sinks_hbm, x_hbm, gain_hbm, w_hbm, b_hbm, cos_hbm, sin_hbm, k_hbm, v_hbm,
                  k_out, v_out, part, q_buf,
                  lens, sinks, todo, ends, x_t, gain, b_qkv, cos_t, sin_t,
                  w_buf, w_f32, acc, h_buf, kn_t, vn_t, k_buf, v_buf, e_buf,
                  small_sem, w_sem, in_sem, out_sem):
    d_model, seqs = x_t.shape
    n_pieces = seqs // PIECE
    rows_in = d_model // PARTS

    smalls = [pltpu.make_async_copy(src, dst, small_sem.at[i]) for i, (src, dst) in enumerate(
        [(x_hbm, x_t), (gain_hbm, gain), (b_hbm, b_qkv), (cos_hbm, cos_t), (sin_hbm, sin_t), (lens_hbm, lens), (sinks_hbm, sinks)])]
    for c in smalls:
        c.start()

    def w_copy(i, c):
        rows = pl.ds(i * rows_in, rows_in)
        return pltpu.make_async_copy(w_hbm.at[rows, :, pl.ds(pl.multiple_of(c * 128, 128), 128)], w_buf.at[c, rows], w_sem.at[i, c])

    def start_w(i):
        each(5, lambda c: w_copy(i, c).start())

    each(AHEAD, start_w)

    def cache_in(a, i):
        rows = pl.ds(i * PIECE, PIECE)
        src, dst = ((k_hbm, k_buf), (v_hbm, v_buf))[a]
        return pltpu.make_async_copy(src.at[rows], dst.at[rows], in_sem.at[a, i])

    def cache_out(a, i):
        rows = pl.ds(i * PIECE, PIECE)
        src, dst = ((k_buf, k_out), (v_buf, v_out))[a]
        return pltpu.make_async_copy(src.at[rows], dst.at[rows], out_sem.at[a, i])

    for c in smalls:
        c.wait()

    base = lax.axis_index("sp") * 128

    ends[0] = 0

    def note(b, count):
        loc = lens[b] - base
        todo[count] = b
        count = count + jnp.where((loc >= 0) & (loc < LANES), 1, 0)
        ends[b // PIECE + 1] = count
        return count

    lax.fori_loop(0, seqs, note, 0)

    def sq_step(i, total):
        xb = x_t[pl.ds(pl.multiple_of(i * rows_in, rows_in), rows_in), :].astype(jnp.float32)
        return total + jnp.sum((xb * xb).reshape(rows_in // 8, 8, seqs), axis=0)

    sq = jnp.sum(lax.fori_loop(0, PARTS, sq_step, jnp.zeros((8, seqs), jnp.float32)), axis=0, keepdims=True)
    inv = jnp.broadcast_to(lax.rsqrt(sq * (1.0 / d_model) + NORM_EPS), (seqs, seqs)).T[:, 0:1]

    def norm_step(i):
        xb = x_t[pl.ds(pl.multiple_of(i * rows_in, rows_in), rows_in), :].astype(jnp.float32).T
        h_buf[i] = (xb * inv * gain[i]).astype(jnp.bfloat16)


    bias = b_qkv[...].astype(jnp.float32)
    for p in range(2):
        for c in range(5):
            for u in range(2):
                acc[p, c, :, u * 128:u * 128 + 128] = jnp.broadcast_to(bias[2 * p + u:2 * p + u + 1, c * 128:c * 128 + 128], (seqs, 128))

    def project(i):
        @pl.when(i + AHEAD < PARTS)
        def _():
            start_w(i + AHEAD)

        @pl.when(i < 2)
        def _():
            each(n_pieces // 2, lambda u: cache_in(0, i * (n_pieces // 2) + u).start())

        @pl.when((i >= 2) & (i < 4))
        def _():
            each(n_pieces // 2, lambda u: cache_in(1, (i - 2) * (n_pieces // 2) + u).start())

        norm_step(i)
        each(5, lambda c: w_copy(i, c).wait())
        rows = i * rows_in

        def column(c):
            w_f32[c % 2] = w_buf[c, pl.ds(rows, rows_in)].reshape(4 * rows_in, 128).astype(jnp.float32)
            for p in range(2):
                w = jnp.concatenate([w_f32[c % 2, pl.ds(2 * p + u, rows_in, stride=4), :].astype(jnp.bfloat16) for u in range(2)], axis=1)
                acc[p, c] += jnp.dot(h_buf[i], w, preferred_element_type=jnp.float32)

        for c in range(5):
            column(c)

    each(PARTS, project)

    lane = lax.broadcasted_iota(jnp.int32, (seqs, 128), 1)
    low = lane < 64
    first_half = (lane & 63) < 32
    cos4 = jnp.concatenate([cos_t[...]] * 4, axis=0).T
    sin4 = jnp.concatenate([sin_t[...]] * 4, axis=0).T
    sin4 = jnp.where(first_half, -sin4, sin4)

    def rotate(t):
        other = jnp.where(first_half, pltpu.roll(t, 96, 1), pltpu.roll(t, 32, 1))
        return t * cos4 + other * sin4

    def halves(p, tile):
        t0 = acc[p, tile, :, LO]
        t1 = acc[p, tile, :, HI]
        return jnp.where(low, t0, pltpu.roll(t1, 64, 1)), jnp.where(low, pltpu.roll(t0, 64, 1), t1)

    for p in range(2):
        def q_step(tile):
            even, odd = halves(p, tile)
            q_buf[p, pl.ds(pl.multiple_of(2 * tile * PITCH, 8), seqs), :] = rotate(even)
            q_buf[p, pl.ds(pl.multiple_of((2 * tile + 1) * PITCH, 8), seqs), :] = rotate(odd)

        each(4, q_step)
        even, odd = halves(p, 4)
        lanes = slice(p * 128, p * 128 + 128)
        kn_t[lanes, :] = rotate(even).T.astype(jnp.bfloat16)
        vn_t[lanes, :] = odd.T.astype(jnp.bfloat16)

    sink_all = jnp.concatenate(sink_table(sinks), axis=0)
    lane256 = lax.broadcasted_iota(jnp.int32, (256, 128), 1)
    def finish(a, buf, new_t):
        def piece(i):
            cache_in(a, i).wait()

            @pl.when(i > 0)
            def _():
                cache_out(a, i - 1).start()

            begin, end = ends[i], ends[i + 1]

            def step(t, carry):
                new = []
                for u in range(NEW):
                    b = todo[jnp.minimum(begin + t * NEW + u, end - 1)]
                    loc = lens[b] - base
                    col = pltpu.roll(new_t[...], lax.rem(loc - b + 2 * LANES, LANES), 1)
                    new.append((b, jnp.where(lane256 == loc, col, buf[b])))
                for b, tile in new:
                    buf[b] = tile
                return carry

            lax.fori_loop(0, (end - begin + NEW - 1) // NEW, step, 0)

        each(n_pieces, piece)
        cache_out(a, n_pieces - 1).start()

    away = (1 - lax.axis_index("sp") // 2) * 2 * GROUP
    finish(0, k_buf, kn_t)

    def score_away(t):
        first = away + t * GROUP
        score_group(first, base, lens, sink_all, q_buf, lambda u: k_buf[first + u], e_buf.at[t], part.at[t])

    each(2, score_away)
    finish(1, v_buf, vn_t)

    def value_away(t):
        first = away + t * GROUP
        value_group(lambda u: v_buf[first + u], e_buf.at[t], part.at[t])

    each(2, value_away)

    def drain(i, carry):
        cache_out(0, i).wait()
        cache_out(1, i).wait()
        return carry

    lax.fori_loop(0, n_pieces, drain, 0)


def local_attention(hidden, seq_lens, rope_cos, rope_sin, k_cache, v_cache, norm_gain, w_qkv, b_qkv, sink_logits):
    seqs, d_model = hidden.shape
    ctx, kv, dim = k_cache.shape[1:]
    k_t = k_cache.transpose(0, 2, 3, 1).reshape(seqs, kv * dim, ctx)
    v_t = v_cache.transpose(0, 2, 3, 1).reshape(seqs, kv * dim, ctx)
    hbm = lambda a: pltpu.with_memory_space_constraint(a, pltpu.HBM)
    vmem = pl.BlockSpec(memory_space=pltpu.VMEM)
    anyw = pl.BlockSpec(memory_space=pltpu.HBM)
    n_chunks = seqs // PIECE
    k_out, v_out, part, q_buf = pl.pallas_call(
        attend_kernel,
        out_shape=(jax.ShapeDtypeStruct(k_t.shape, k_t.dtype), jax.ShapeDtypeStruct(v_t.shape, v_t.dtype),
                   jax.ShapeDtypeStruct((2, GROUP * 8 + 8, kv * dim), jnp.float32),
                   jax.ShapeDtypeStruct((2, 8 * PITCH, 128), jnp.float32)),
        in_specs=[anyw] * 10,
        out_specs=(anyw, anyw, vmem, vmem),
        scratch_shapes=[
            pltpu.SMEM((seqs,), jnp.int32),
            pltpu.SMEM((kv * 8,), jnp.float32),
            pltpu.SMEM((seqs + NEW,), jnp.int32),
            pltpu.SMEM((seqs // PIECE + 1,), jnp.int32),
            pltpu.VMEM((d_model, seqs), jnp.bfloat16),
            pltpu.VMEM((PARTS, 1, d_model // PARTS), jnp.float32),
            pltpu.VMEM(b_qkv.shape, jnp.bfloat16),
            pltpu.VMEM((dim // 2, seqs), jnp.float32),
            pltpu.VMEM((dim // 2, seqs), jnp.float32),
            pltpu.VMEM((5, d_model, kv, 128), jnp.bfloat16),
            pltpu.VMEM((2, d_model // PARTS * kv, 128), jnp.float32),
            pltpu.VMEM((2, 5, seqs, 256), jnp.float32),
            pltpu.VMEM((PARTS, seqs, d_model // PARTS), jnp.bfloat16),
            pltpu.VMEM((kv * dim, seqs), jnp.bfloat16),
            pltpu.VMEM((kv * dim, seqs), jnp.bfloat16),
            pltpu.VMEM(k_t.shape, jnp.bfloat16),
            pltpu.VMEM(v_t.shape, jnp.bfloat16),
            pltpu.VMEM((2, GROUP * 32, 128), jnp.bfloat16),
            pltpu.SemaphoreType.DMA((7,)),
            pltpu.SemaphoreType.DMA((PARTS, 5)),
            pltpu.SemaphoreType.DMA((2, n_chunks)),
            pltpu.SemaphoreType.DMA((2, n_chunks)),
        ],
        compiler_params=pltpu.CompilerParams(vmem_limit_bytes=44 * 1024 * 1024),
        cost_estimate=pl.CostEstimate(flops=3 * 10**9, bytes_accessed=48 * 10**6, transcendentals=10**6),
    )(hbm(seq_lens), hbm(sink_logits), hbm(hidden.T), norm_gain, hbm(w_qkv), hbm(b_qkv),
      hbm(rope_cos.T), hbm(rope_sin.T), hbm(k_t), hbm(v_t))
    return k_out, v_out, part, q_buf


def exchange_kernel(part, q_buf, k_hbm, v_hbm, lens_hbm, sinks_hbm, bias, w_hbm, y_out,
                    lens, sinks, k_buf, v_buf, e_buf, mine_part, w_buf, from_core, to_chip, own, from_chip, o_all, lhs, y_buf, from_tp, gather,
                    small_sem, kv_sem, w_sem, core_send, core_recv, chip_send, chip_recv, o_send, o_recv, tp_send, tp_recv, ag_send, ag_recv):
    tp = lax.axis_index("tp")
    sp = lax.axis_index("sp")
    core = lax.rem(sp, 2)
    chip = sp // 2
    width = gather.shape[-1]
    share = w_buf.shape[0]
    sibling = {"sp": sp + 1 - 2 * core}
    across_x = {"sp": lax.rem(sp + 2, 4)}
    across_y = {"tp": 1 - tp}

    smalls = [pltpu.make_async_copy(sinks_hbm, sinks, small_sem.at[0]), pltpu.make_async_copy(lens_hbm, lens, small_sem.at[1])]
    first_own = pl.multiple_of(chip * 2 * GROUP, GROUP)
    kv_copies = [[pltpu.make_async_copy(src.at[pl.ds(first_own + t * GROUP, GROUP)], dst.at[pl.ds(t * GROUP, GROUP)], kv_sem.at[a, t]) for t in range(2)]
                 for a, (src, dst) in enumerate(((k_hbm, k_buf), (v_hbm, v_buf)))]
    for c in smalls + kv_copies[0] + kv_copies[1]:
        c.start()
    w_copies = [pltpu.make_async_copy(w_hbm.at[pl.ds((share * core + i) * width, width)], w_buf.at[i], w_sem.at[i]) for i in range(share)]
    for c in w_copies:
        c.start()

    barrier = pltpu.get_barrier_semaphore()
    for peer in (sibling, across_x, across_y):
        pl.semaphore_signal(barrier, inc=1, device_id=peer, device_id_type=MESH)
    pl.semaphore_wait(barrier, 3)

    def remote(src, dst, ss, rs, peer):
        return pltpu.make_async_remote_copy(src_ref=src, dst_ref=dst, send_sem=ss, recv_sem=rs, device_id=peer, device_id_type=MESH)

    pieces = [(0, 8), (8, 16), (16, 24), (24, 32)]
    order = [3, 0, 1, 2]

    def piece_rows(i):
        j0, j1 = pieces[i]
        return pl.ds(8 * j0, 8 * (j1 - j0) + (8 if i == len(pieces) - 1 else 0))

    away_theirs = part.at[1 - core]
    core_copies = [remote(away_theirs.at[piece_rows(i)], from_core.at[0, piece_rows(i)], core_send.at[i], core_recv.at[i], sibling) for i in range(4)]
    for i in order:
        core_copies[i].start()

    lane = lax.broadcasted_iota(jnp.int32, (8, 128), 1)
    high = lane // 64

    def spread(f, j, p):
        return jnp.take_along_axis(f, j * 4 + 2 * p + high, axis=1)

    def stats(a, b):
        m_a, s_a = a[0], a[1]
        m_b, s_b = b[0], b[1]
        m = jnp.maximum(m_a, m_b)
        f_a = jnp.exp(m_a - m)
        f_b = jnp.exp(m_b - m)
        return m, s_a * f_a + s_b * f_b, f_a, f_b

    def stat_rows(ref):
        return ref[STAT, LO], ref[STAT, HI]

    def merge(a_ref, b_ref, out_ref, f_a, f_b, j0, j1):
        for j in range(j0, j1):
            rows = slice(8 * j, 8 * j + 8)
            for p in range(2):
                cols = slice(128 * p, 128 * p + 128)
                out_ref[rows, cols] = a_ref[rows, cols] * spread(f_a, j, p) + b_ref[rows, cols] * spread(f_b, j, p)

    core_copies[3].wait_recv()
    away = part.at[core]
    m, s, f_a, f_b = stats(stat_rows(away), stat_rows(from_core.at[0]))
    to_chip[STAT, LO] = m
    to_chip[STAT, HI] = s
    chip_copies = [remote(to_chip.at[piece_rows(i)], from_chip.at[piece_rows(i)], chip_send.at[i], chip_recv.at[i], across_x) for i in range(len(pieces))]
    for i in order:
        if i != 3:
            core_copies[i].wait_recv()
        merge(away, from_core.at[0], to_chip, f_a, f_b, *pieces[i])
        chip_copies[i].start()

    for c in smalls:
        c.wait()
    base = sp * 128
    sink_rows = sink_table(sinks)
    sink_all = jnp.concatenate(sink_rows, axis=0)
    for c in kv_copies[0]:
        c.wait()
    each(2, lambda t: score_group(first_own + t * GROUP, base, lens, sink_all, q_buf, lambda u: k_buf[t * GROUP + u], e_buf.at[t], mine_part.at[t]))
    for c in kv_copies[1]:
        c.wait()
    each(2, lambda t: value_group(lambda u: v_buf[t * GROUP + u], e_buf.at[t], mine_part.at[t]))
    core_copies.append(remote(mine_part.at[1 - core], from_core.at[1], core_send.at[4], core_recv.at[4], sibling))
    core_copies[4].start()

    sink = sink_rows[3]
    for k in range(3):
        sink = jnp.where((lane & 3) == k, sink_rows[k], sink)

    core_copies[4].wait_recv()
    here = mine_part.at[core]
    m_own, s_own, f_a, f_b = stats(stat_rows(here), stat_rows(from_core.at[1]))
    merge(here, from_core.at[1], own, f_a, f_b, 0, 32)

    chip_copies[3].wait_recv()
    m, s, f_a, f_b = stats((m_own, s_own), stat_rows(from_chip))
    scale = 1.0 / (s + jnp.exp(sink - m))
    f_a = f_a * scale
    f_b = f_b * scale
    o_copies = []
    for i in order:
        if i != 3:
            chip_copies[i].wait_recv()
        for j in range(*pieces[i]):
            rows = slice(8 * j, 8 * j + 8)
            for p in range(2):
                cols = slice(128 * p, 128 * p + 128)
                o_all[core, p, rows, :] = own[rows, cols] * spread(f_a, j, p) + from_chip[rows, cols] * spread(f_b, j, p)
        rows = pl.ds(8 * pieces[i][0], 8 * 8)
        c = remote(o_all.at[core, :, rows], o_all.at[core, :, rows], o_send.at[i], o_recv.at[i], sibling)
        c.start()
        o_copies.append(c)

    low = lax.broadcasted_iota(jnp.int32, (GROUP, 128), 1) < 64

    def fill_lhs(g):
        rows = pl.ds(pl.multiple_of(g * GROUP, GROUP), GROUP)
        for p in range(2):
            for t in range(4):
                a = o_all[g, p, pl.ds(2 * t, GROUP, stride=8), :]
                b = o_all[g, p, pl.ds(2 * t + 1, GROUP, stride=8), :]
                even_k = (2 * p) * 512 + t * 128
                odd_k = (2 * p + 1) * 512 + t * 128
                lhs[rows, even_k:even_k + 128] = jnp.where(low, a, pltpu.roll(b, 64, 1)).astype(jnp.bfloat16)
                lhs[rows, odd_k:odd_k + 128] = jnp.where(low, pltpu.roll(a, 64, 1), b).astype(jnp.bfloat16)

    fill_lhs(core)
    for c in o_copies:
        c.wait_recv()
    fill_lhs(1 - core)

    theirs = pl.ds(pl.multiple_of((1 - tp) * GROUP, GROUP), GROUP)
    mine = pl.ds(pl.multiple_of(tp * GROUP, GROUP), GROUP)
    tp_copies = []
    for i in range(share):
        w_copies[i].wait()
        y_buf[i] = lax.dot_general(lhs[...], w_buf[i], (((1,), (1,)), ((), ())), preferred_element_type=jnp.float32)
        c = remote(y_buf.at[i, theirs], from_tp.at[i], tp_send.at[i], tp_recv.at[i], across_y)
        c.start()
        tp_copies.append(c)

    started = []

    def piece(t, x, block):
        return gather.at[block, pl.ds(pl.multiple_of(x * 2 * GROUP + t * GROUP, GROUP), GROUP)]

    def send(ref, slot, i, peer):
        c = remote(ref, ref, ag_send.at[slot, i], ag_recv.at[slot, i], peer)
        c.start()
        started.append(c)

    def arrived(ref, slot, i):
        remote(ref, ref, ag_send.at[slot, i], ag_recv.at[slot, i], sibling).wait_recv()

    block = [share * core + i for i in range(share)]
    for i in range(share):
        tp_copies[i].wait_recv()
        gather[block[i], pl.ds(pl.multiple_of(chip * 2 * GROUP + tp * GROUP, GROUP), GROUP), :] = y_buf[i, mine] + from_tp[i] + bias[block[i]]
        ref = piece(tp, chip, block[i])
        send(ref, 1, i, across_y)
        send(ref, 0, i, across_x)
        send(ref, 4, i, sibling)
    for i in range(share):
        arrived(piece(1 - tp, chip, block[i]), 1, i)
        send(piece(1 - tp, chip, block[i]), 2, i, across_x)
        send(piece(1 - tp, chip, block[i]), 6, i, sibling)
        arrived(piece(tp, 1 - chip, block[i]), 0, i)
        send(piece(tp, 1 - chip, block[i]), 5, i, sibling)

    def turn(b):
        y_out[pl.ds(pl.multiple_of(b * width, width), width), :] = gather[b].T

    for i in range(share):
        arrived(piece(1 - tp, 1 - chip, block[i]), 2, i)
        send(piece(1 - tp, 1 - chip, block[i]), 3, i, sibling)
        turn(block[i])
    for i in range(share):
        other = share * (1 - core) + i
        arrived(piece(tp, chip, other), 4, i)
        arrived(piece(tp, 1 - chip, other), 5, i)
        arrived(piece(1 - tp, chip, other), 6, i)
        arrived(piece(1 - tp, 1 - chip, other), 3, i)
        turn(other)
    for c in core_copies + chip_copies + o_copies + tp_copies + started:
        c.wait_send()


def exchange(part, q_buf, k_out, v_out, seq_lens, sink_logits, w_o, bias):
    heads, d_out = w_o.shape
    n_col = bias.shape[0]
    cols = d_out // n_col
    share = n_col // 2
    hbm = lambda a: pltpu.with_memory_space_constraint(a, pltpu.HBM)
    vmem = pl.BlockSpec(memory_space=pltpu.VMEM)
    anyw = pl.BlockSpec(memory_space=pltpu.HBM)
    block = part.shape[1:]
    dma = pltpu.SemaphoreType.DMA
    return pl.pallas_call(
        exchange_kernel,
        out_shape=jax.ShapeDtypeStruct((d_out, 128), jnp.float32),
        in_specs=[vmem, vmem, anyw, anyw, anyw, anyw, vmem, anyw],
        out_specs=vmem,
        scratch_shapes=[
            pltpu.SMEM(seq_lens.shape, jnp.int32),
            pltpu.SMEM(sink_logits.shape, jnp.float32),
            pltpu.VMEM((2 * GROUP,) + k_out.shape[1:], jnp.bfloat16),
            pltpu.VMEM((2 * GROUP,) + k_out.shape[1:], jnp.bfloat16),
            pltpu.VMEM((2, GROUP * 32, 128), jnp.bfloat16),
            pltpu.VMEM((2,) + block, jnp.float32),
            pltpu.VMEM((share, cols, heads), jnp.bfloat16),
            pltpu.VMEM((2,) + block, jnp.float32),
            pltpu.VMEM(block, jnp.float32),
            pltpu.VMEM(block, jnp.float32),
            pltpu.VMEM(block, jnp.float32),
            pltpu.VMEM((2, 2, 256, 128), jnp.float32),
            pltpu.VMEM((2 * GROUP, heads), jnp.bfloat16),
            pltpu.VMEM((share, 2 * GROUP, cols), jnp.float32),
            pltpu.VMEM((share, GROUP, cols), jnp.float32),
            pltpu.VMEM((n_col, 128, cols), jnp.float32),
            dma((2,)), dma((2, 2)), dma((share,)), dma((5,)), dma((5,)), dma((4,)), dma((4,)), dma((4,)), dma((4,)), dma((share,)), dma((share,)),
            dma((7, share)), dma((7, share)),
        ],
        compiler_params=pltpu.CompilerParams(collective_id=0, has_side_effects=True, vmem_limit_bytes=40 * 1024 * 1024),
        cost_estimate=pl.CostEstimate(flops=4 * 10**8, bytes_accessed=16 * 10**6, transcendentals=10**5),
      )(part, q_buf, hbm(k_out), hbm(v_out), hbm(seq_lens), hbm(sink_logits), bias, hbm(w_o.T))


def solution(mesh):
    cache_spec = P("dp", "sp", "tp", None)

    def block_step(hidden, seq_lens, rope_cos, rope_sin, k_cache, v_cache, norm_gain, w_qkv, b_qkv, sink_logits, w_o, b_o):
        d_model = hidden.shape[1]
        gain = norm_gain.astype(jnp.float32).reshape(PARTS, 1, d_model // PARTS)
        bias = b_o.astype(jnp.float32).reshape(BLOCKS, 1, d_model // BLOCKS)
        k_out, v_out, part, q_buf = local_attention(hidden, seq_lens, rope_cos, rope_sin, k_cache, v_cache, gain, w_qkv, b_qkv, sink_logits)
        y_t = exchange(part, q_buf, k_out, v_out, seq_lens, sink_logits, w_o, bias)
        out_hidden = (hidden.T.astype(jnp.float32) + y_t).astype(jnp.bfloat16).T
        seqs, ctx, kv, dim = k_cache.shape
        back = lambda a: a.reshape(seqs, kv, dim, ctx).transpose(0, 3, 1, 2)
        return out_hidden, back(k_out), back(v_out)

    return jax.shard_map(block_step, mesh=mesh, in_specs=(P("dp", None), P("dp"), P("dp", None), P("dp", None), cache_spec, cache_spec, P(None), P(None, "tp", None), P("tp", None), P("tp"), P("tp", None), P(None)), out_specs=(P("dp", None), cache_spec, cache_spec), check_vma=False)
```

```python
import functools
import jax
import jax.numpy as jnp
from jax import lax
from jax.sharding import PartitionSpec as P
from jax.experimental import pallas as pl
from jax.experimental.pallas import tpu as pltpu

NORM_EPS = 1e-5
GROUP = 32
LANES = 128
LO = slice(0, LANES)
HI = slice(LANES, 2 * LANES)
STAT = slice(8 * GROUP, 8 * GROUP + 8)
PIECE = 32
AHEAD = 3
PITCH = 136
NEW = 8
PARTS = 6
BLOCKS = 6
MESH = pl.DeviceIdType.MESH


def each(n, fn):
    def step(i, carry):
        fn(i)
        return carry
    lax.fori_loop(0, n, step, 0)


def sink_table(sinks):
    row = lax.broadcasted_iota(jnp.int32, (8, 128), 0)
    rows = []
    for k in range(4):
        t = jnp.zeros((8, 128), jnp.float32)
        for g in range(8):
            t = jnp.where(row == g, sinks[k * 8 + g], t)
        rows.append(t)
    return rows


def score_group(first, base, lens, sink_all, q_buf, keys, e_buf, out):
    lane8 = lax.broadcasted_iota(jnp.int32, (8, 128), 1)
    lane32 = lax.broadcasted_iota(jnp.int32, (32, 128), 1)
    q_lane = lax.broadcasted_iota(jnp.int32, (8, 256), 1) // 64
    m_acc = jnp.zeros((8, 128), jnp.float32)
    s_acc = jnp.zeros((8, 128), jnp.float32)
    for u in range(GROUP):
        b = first + u
        rows = jnp.concatenate([q_buf[p, pl.ds(b, 8, stride=PITCH), :] for p in range(2)], axis=1)
        q_blk = jnp.concatenate([jnp.where(q_lane == k, rows, 0.0) for k in range(4)], axis=0).astype(jnp.bfloat16)
        logits = jnp.dot(q_blk, keys(u), preferred_element_type=jnp.float32) * 0.125
        logits = jnp.where(lane32 <= lens[b] - base, logits, -jnp.inf)
        m = jnp.maximum(jnp.broadcast_to(jnp.max(logits, axis=1, keepdims=True), logits.shape), sink_all)
        e = jnp.exp(logits - m)
        s = jnp.sum(e, axis=1, keepdims=True)
        e_buf[32 * u:32 * u + 32, :] = e.astype(jnp.bfloat16)
        for k in range(4):
            here = lane8 == u * 4 + k
            m_acc = jnp.where(here, m[8 * k:8 * k + 8], m_acc)
            s_acc = jnp.where(here, s[8 * k:8 * k + 8], s_acc)
    out[STAT, LO] = m_acc
    out[STAT, HI] = s_acc


def value_group(values, e_buf, out):
    half8 = lax.broadcasted_iota(jnp.int32, (8, 128), 1) < 64
    for u in range(GROUP):
        r = lax.dot_general(e_buf[32 * u:32 * u + 32, :], values(u), (((1,), (1,)), ((), ())), preferred_element_type=jnp.float32)
        out[8 * u:8 * u + 8, LO] = jnp.where(half8, r[0:8, LO], r[8:16, LO])
        out[8 * u:8 * u + 8, HI] = jnp.where(half8, r[16:24, HI], r[24:32, HI])


def attend_kernel(lens_hbm, sinks_hbm, x_hbm, gain_hbm, w_hbm, b_hbm, cos_hbm, sin_hbm, k_hbm, v_hbm,
                  k_out, v_out, part, q_buf,
                  lens, sinks, todo, ends, x_t, gain, b_qkv, cos_t, sin_t,
                  w_buf, w_f32, acc, h_buf, kn_t, vn_t, k_buf, v_buf, e_buf,
                  small_sem, w_sem, in_sem, out_sem):
    d_model, seqs = x_t.shape
    n_pieces = seqs // PIECE
    rows_in = d_model // PARTS

    smalls = [pltpu.make_async_copy(src, dst, small_sem.at[i]) for i, (src, dst) in enumerate(
        [(x_hbm, x_t), (gain_hbm, gain), (b_hbm, b_qkv), (cos_hbm, cos_t), (sin_hbm, sin_t), (lens_hbm, lens), (sinks_hbm, sinks)])]
    for c in smalls:
        c.start()

    def w_copy(i, c):
        rows = pl.ds(i * rows_in, rows_in)
        return pltpu.make_async_copy(w_hbm.at[rows, :, pl.ds(pl.multiple_of(c * 128, 128), 128)], w_buf.at[c, rows], w_sem.at[i, c])

    def start_w(i):
        each(5, lambda c: w_copy(i, c).start())

    each(AHEAD, start_w)

    def cache_in(a, i):
        rows = pl.ds(i * PIECE, PIECE)
        src, dst = ((k_hbm, k_buf), (v_hbm, v_buf))[a]
        return pltpu.make_async_copy(src.at[rows], dst.at[rows], in_sem.at[a, i])

    def cache_out(a, i):
        rows = pl.ds(i * PIECE, PIECE)
        src, dst = ((k_buf, k_out), (v_buf, v_out))[a]
        return pltpu.make_async_copy(src.at[rows], dst.at[rows], out_sem.at[a, i])

    for c in smalls:
        c.wait()

    base = lax.axis_index("sp") * 128

    ends[0] = 0

    def note(b, count):
        loc = lens[b] - base
        todo[count] = b
        count = count + jnp.where((loc >= 0) & (loc < LANES), 1, 0)
        ends[b // PIECE + 1] = count
        return count

    lax.fori_loop(0, seqs, note, 0)

    def sq_step(i, total):
        xb = x_t[pl.ds(pl.multiple_of(i * rows_in, rows_in), rows_in), :].astype(jnp.float32)
        return total + jnp.sum((xb * xb).reshape(rows_in // 8, 8, seqs), axis=0)

    sq = jnp.sum(lax.fori_loop(0, PARTS, sq_step, jnp.zeros((8, seqs), jnp.float32)), axis=0, keepdims=True)
    inv = jnp.broadcast_to(lax.rsqrt(sq * (1.0 / d_model) + NORM_EPS), (seqs, seqs)).T[:, 0:1]

    def norm_step(i):
        xb = x_t[pl.ds(pl.multiple_of(i * rows_in, rows_in), rows_in), :].astype(jnp.float32).T
        h_buf[i] = (xb * inv * gain[i]).astype(jnp.bfloat16)


    bias = b_qkv[...].astype(jnp.float32)
    for p in range(2):
        for c in range(5):
            for u in range(2):
                acc[p, c, :, u * 128:u * 128 + 128] = jnp.broadcast_to(bias[2 * p + u:2 * p + u + 1, c * 128:c * 128 + 128], (seqs, 128))

    def project(i):
        @pl.when(i + AHEAD < PARTS)
        def _():
            start_w(i + AHEAD)

        @pl.when(i < 2)
        def _():
            each(n_pieces // 2, lambda u: cache_in(0, i * (n_pieces // 2) + u).start())

        @pl.when((i >= 2) & (i < 4))
        def _():
            each(n_pieces // 2, lambda u: cache_in(1, (i - 2) * (n_pieces // 2) + u).start())

        norm_step(i)
        each(5, lambda c: w_copy(i, c).wait())
        rows = i * rows_in

        def column(c):
            w_f32[c % 2] = w_buf[c, pl.ds(rows, rows_in)].reshape(4 * rows_in, 128).astype(jnp.float32)
            for p in range(2):
                w = jnp.concatenate([w_f32[c % 2, pl.ds(2 * p + u, rows_in, stride=4), :].astype(jnp.bfloat16) for u in range(2)], axis=1)
                acc[p, c] += jnp.dot(h_buf[i], w, preferred_element_type=jnp.float32)

        for c in range(5):
            column(c)

    each(PARTS, project)

    lane = lax.broadcasted_iota(jnp.int32, (seqs, 128), 1)
    low = lane < 64
    first_half = (lane & 63) < 32
    cos4 = jnp.concatenate([cos_t[...]] * 4, axis=0).T
    sin4 = jnp.concatenate([sin_t[...]] * 4, axis=0).T
    sin4 = jnp.where(first_half, -sin4, sin4)

    def rotate(t):
        other = jnp.where(first_half, pltpu.roll(t, 96, 1), pltpu.roll(t, 32, 1))
        return t * cos4 + other * sin4

    def halves(p, tile):
        t0 = acc[p, tile, :, LO]
        t1 = acc[p, tile, :, HI]
        return jnp.where(low, t0, pltpu.roll(t1, 64, 1)), jnp.where(low, pltpu.roll(t0, 64, 1), t1)

    for p in range(2):
        def q_step(tile):
            even, odd = halves(p, tile)
            q_buf[p, pl.ds(pl.multiple_of(2 * tile * PITCH, 8), seqs), :] = rotate(even)
            q_buf[p, pl.ds(pl.multiple_of((2 * tile + 1) * PITCH, 8), seqs), :] = rotate(odd)

        each(4, q_step)
        even, odd = halves(p, 4)
        lanes = slice(p * 128, p * 128 + 128)
        kn_t[lanes, :] = rotate(even).T.astype(jnp.bfloat16)
        vn_t[lanes, :] = odd.T.astype(jnp.bfloat16)

    sink_all = jnp.concatenate(sink_table(sinks), axis=0)
    lane256 = lax.broadcasted_iota(jnp.int32, (256, 128), 1)
    def finish(a, buf, new_t):
        def piece(i):
            cache_in(a, i).wait()

            @pl.when(i > 0)
            def _():
                cache_out(a, i - 1).start()

            begin, end = ends[i], ends[i + 1]

            def step(t, carry):
                new = []
                for u in range(NEW):
                    b = todo[jnp.minimum(begin + t * NEW + u, end - 1)]
                    loc = lens[b] - base
                    col = pltpu.roll(new_t[...], lax.rem(loc - b + 2 * LANES, LANES), 1)
                    new.append((b, jnp.where(lane256 == loc, col, buf[b])))
                for b, tile in new:
                    buf[b] = tile
                return carry

            lax.fori_loop(0, (end - begin + NEW - 1) // NEW, step, 0)

        each(n_pieces, piece)
        cache_out(a, n_pieces - 1).start()

    away = (1 - lax.axis_index("sp") // 2) * 2 * GROUP
    finish(0, k_buf, kn_t)

    def score_away(t):
        first = away + t * GROUP
        score_group(first, base, lens, sink_all, q_buf, lambda u: k_buf[first + u], e_buf.at[t], part.at[t])

    each(2, score_away)
    finish(1, v_buf, vn_t)

    def value_away(t):
        first = away + t * GROUP
        value_group(lambda u: v_buf[first + u], e_buf.at[t], part.at[t])

    each(2, value_away)

    def drain(i, carry):
        cache_out(0, i).wait()
        cache_out(1, i).wait()
        return carry

    lax.fori_loop(0, n_pieces, drain, 0)


def local_attention(hidden, seq_lens, rope_cos, rope_sin, k_cache, v_cache, norm_gain, w_qkv, b_qkv, sink_logits):
    seqs, d_model = hidden.shape
    ctx, kv, dim = k_cache.shape[1:]
    k_t = k_cache.transpose(0, 2, 3, 1).reshape(seqs, kv * dim, ctx)
    v_t = v_cache.transpose(0, 2, 3, 1).reshape(seqs, kv * dim, ctx)
    hbm = lambda a: pltpu.with_memory_space_constraint(a, pltpu.HBM)
    vmem = pl.BlockSpec(memory_space=pltpu.VMEM)
    anyw = pl.BlockSpec(memory_space=pltpu.HBM)
    n_chunks = seqs // PIECE
    k_out, v_out, part, q_buf = pl.pallas_call(
        attend_kernel,
        out_shape=(jax.ShapeDtypeStruct(k_t.shape, k_t.dtype), jax.ShapeDtypeStruct(v_t.shape, v_t.dtype),
                   jax.ShapeDtypeStruct((2, GROUP * 8 + 8, kv * dim), jnp.float32),
                   jax.ShapeDtypeStruct((2, 8 * PITCH, 128), jnp.float32)),
        in_specs=[anyw] * 10,
        out_specs=(anyw, anyw, vmem, vmem),
        scratch_shapes=[
            pltpu.SMEM((seqs,), jnp.int32),
            pltpu.SMEM((kv * 8,), jnp.float32),
            pltpu.SMEM((seqs + NEW,), jnp.int32),
            pltpu.SMEM((seqs // PIECE + 1,), jnp.int32),
            pltpu.VMEM((d_model, seqs), jnp.bfloat16),
            pltpu.VMEM((PARTS, 1, d_model // PARTS), jnp.float32),
            pltpu.VMEM(b_qkv.shape, jnp.bfloat16),
            pltpu.VMEM((dim // 2, seqs), jnp.float32),
            pltpu.VMEM((dim // 2, seqs), jnp.float32),
            pltpu.VMEM((5, d_model, kv, 128), jnp.bfloat16),
            pltpu.VMEM((2, d_model // PARTS * kv, 128), jnp.float32),
            pltpu.VMEM((2, 5, seqs, 256), jnp.float32),
            pltpu.VMEM((PARTS, seqs, d_model // PARTS), jnp.bfloat16),
            pltpu.VMEM((kv * dim, seqs), jnp.bfloat16),
            pltpu.VMEM((kv * dim, seqs), jnp.bfloat16),
            pltpu.VMEM(k_t.shape, jnp.bfloat16),
            pltpu.VMEM(v_t.shape, jnp.bfloat16),
            pltpu.VMEM((2, GROUP * 32, 128), jnp.bfloat16),
            pltpu.SemaphoreType.DMA((7,)),
            pltpu.SemaphoreType.DMA((PARTS, 5)),
            pltpu.SemaphoreType.DMA((2, n_chunks)),
            pltpu.SemaphoreType.DMA((2, n_chunks)),
        ],
        compiler_params=pltpu.CompilerParams(vmem_limit_bytes=44 * 1024 * 1024),
        cost_estimate=pl.CostEstimate(flops=3 * 10**9, bytes_accessed=48 * 10**6, transcendentals=10**6),
    )(hbm(seq_lens), hbm(sink_logits), hbm(hidden.T), norm_gain, hbm(w_qkv), hbm(b_qkv),
      hbm(rope_cos.T), hbm(rope_sin.T), hbm(k_t), hbm(v_t))
    return k_out, v_out, part, q_buf


def exchange_kernel(part, q_buf, k_hbm, v_hbm, lens_hbm, sinks_hbm, bias, w_hbm, y_out,
                    lens, sinks, k_buf, v_buf, e_buf, mine_part, w_buf, from_core, to_chip, own, from_chip, o_all, lhs, y_buf, from_tp, gather,
                    small_sem, kv_sem, w_sem, core_send, core_recv, chip_send, chip_recv, o_send, o_recv, tp_send, tp_recv, ag_send, ag_recv):
    tp = lax.axis_index("tp")
    sp = lax.axis_index("sp")
    core = lax.rem(sp, 2)
    chip = sp // 2
    width = gather.shape[-1]
    share = w_buf.shape[0]
    sibling = {"sp": sp + 1 - 2 * core}
    across_x = {"sp": lax.rem(sp + 2, 4)}
    across_y = {"tp": 1 - tp}

    smalls = [pltpu.make_async_copy(sinks_hbm, sinks, small_sem.at[0]), pltpu.make_async_copy(lens_hbm, lens, small_sem.at[1])]
    first_own = pl.multiple_of(chip * 2 * GROUP, GROUP)
    kv_copies = [[pltpu.make_async_copy(src.at[pl.ds(first_own + t * GROUP, GROUP)], dst.at[pl.ds(t * GROUP, GROUP)], kv_sem.at[a, t]) for t in range(2)]
                 for a, (src, dst) in enumerate(((k_hbm, k_buf), (v_hbm, v_buf)))]
    for c in smalls + kv_copies[0] + kv_copies[1]:
        c.start()
    w_copies = [pltpu.make_async_copy(w_hbm.at[pl.ds((share * core + i) * width, width)], w_buf.at[i], w_sem.at[i]) for i in range(share)]
    for c in w_copies:
        c.start()

    barrier = pltpu.get_barrier_semaphore()
    for peer in (sibling, across_x, across_y):
        pl.semaphore_signal(barrier, inc=1, device_id=peer, device_id_type=MESH)
    pl.semaphore_wait(barrier, 3)

    def remote(src, dst, ss, rs, peer):
        return pltpu.make_async_remote_copy(src_ref=src, dst_ref=dst, send_sem=ss, recv_sem=rs, device_id=peer, device_id_type=MESH)

    pieces = [(0, 8), (8, 16), (16, 24), (24, 32)]
    order = [3, 0, 1, 2]

    def piece_rows(i):
        j0, j1 = pieces[i]
        return pl.ds(8 * j0, 8 * (j1 - j0) + (8 if i == len(pieces) - 1 else 0))

    away_theirs = part.at[1 - core]
    core_copies = [remote(away_theirs.at[piece_rows(i)], from_core.at[0, piece_rows(i)], core_send.at[i], core_recv.at[i], sibling) for i in range(4)]
    for i in order:
        core_copies[i].start()

    lane = lax.broadcasted_iota(jnp.int32, (8, 128), 1)
    high = lane // 64

    def spread(f, j, p):
        return jnp.take_along_axis(f, j * 4 + 2 * p + high, axis=1)

    def stats(a, b):
        m_a, s_a = a[0], a[1]
        m_b, s_b = b[0], b[1]
        m = jnp.maximum(m_a, m_b)
        f_a = jnp.exp(m_a - m)
        f_b = jnp.exp(m_b - m)
        return m, s_a * f_a + s_b * f_b, f_a, f_b

    def stat_rows(ref):
        return ref[STAT, LO], ref[STAT, HI]

    def merge(a_ref, b_ref, out_ref, f_a, f_b, j0, j1):
        for j in range(j0, j1):
            rows = slice(8 * j, 8 * j + 8)
            for p in range(2):
                cols = slice(128 * p, 128 * p + 128)
                out_ref[rows, cols] = a_ref[rows, cols] * spread(f_a, j, p) + b_ref[rows, cols] * spread(f_b, j, p)

    core_copies[3].wait_recv()
    away = part.at[core]
    m, s, f_a, f_b = stats(stat_rows(away), stat_rows(from_core.at[0]))
    to_chip[STAT, LO] = m
    to_chip[STAT, HI] = s
    chip_copies = [remote(to_chip.at[piece_rows(i)], from_chip.at[piece_rows(i)], chip_send.at[i], chip_recv.at[i], across_x) for i in range(len(pieces))]
    for i in order:
        if i != 3:
            core_copies[i].wait_recv()
        merge(away, from_core.at[0], to_chip, f_a, f_b, *pieces[i])
        chip_copies[i].start()

    for c in smalls:
        c.wait()
    base = sp * 128
    sink_rows = sink_table(sinks)
    sink_all = jnp.concatenate(sink_rows, axis=0)
    for c in kv_copies[0]:
        c.wait()
    each(2, lambda t: score_group(first_own + t * GROUP, base, lens, sink_all, q_buf, lambda u: k_buf[t * GROUP + u], e_buf.at[t], mine_part.at[t]))
    for c in kv_copies[1]:
        c.wait()
    each(2, lambda t: value_group(lambda u: v_buf[t * GROUP + u], e_buf.at[t], mine_part.at[t]))
    core_copies.append(remote(mine_part.at[1 - core], from_core.at[1], core_send.at[4], core_recv.at[4], sibling))
    core_copies[4].start()

    sink = sink_rows[3]
    for k in range(3):
        sink = jnp.where((lane & 3) == k, sink_rows[k], sink)

    core_copies[4].wait_recv()
    here = mine_part.at[core]
    m_own, s_own, f_a, f_b = stats(stat_rows(here), stat_rows(from_core.at[1]))
    merge(here, from_core.at[1], own, f_a, f_b, 0, 32)

    chip_copies[3].wait_recv()
    m, s, f_a, f_b = stats((m_own, s_own), stat_rows(from_chip))
    scale = 1.0 / (s + jnp.exp(sink - m))
    f_a = f_a * scale
    f_b = f_b * scale
    o_copies = []
    for i in order:
        if i != 3:
            chip_copies[i].wait_recv()
        for j in range(*pieces[i]):
            rows = slice(8 * j, 8 * j + 8)
            for p in range(2):
                cols = slice(128 * p, 128 * p + 128)
                o_all[core, p, rows, :] = own[rows, cols] * spread(f_a, j, p) + from_chip[rows, cols] * spread(f_b, j, p)
        rows = pl.ds(8 * pieces[i][0], 8 * 8)
        c = remote(o_all.at[core, :, rows], o_all.at[core, :, rows], o_send.at[i], o_recv.at[i], sibling)
        c.start()
        o_copies.append(c)

    low = lax.broadcasted_iota(jnp.int32, (GROUP, 128), 1) < 64

    def fill_lhs(g):
        rows = pl.ds(pl.multiple_of(g * GROUP, GROUP), GROUP)
        for p in range(2):
            for t in range(4):
                a = o_all[g, p, pl.ds(2 * t, GROUP, stride=8), :]
                b = o_all[g, p, pl.ds(2 * t + 1, GROUP, stride=8), :]
                even_k = (2 * p) * 512 + t * 128
                odd_k = (2 * p + 1) * 512 + t * 128
                lhs[rows, even_k:even_k + 128] = jnp.where(low, a, pltpu.roll(b, 64, 1)).astype(jnp.bfloat16)
                lhs[rows, odd_k:odd_k + 128] = jnp.where(low, pltpu.roll(a, 64, 1), b).astype(jnp.bfloat16)

    fill_lhs(core)
    for c in o_copies:
        c.wait_recv()
    fill_lhs(1 - core)

    theirs = pl.ds(pl.multiple_of((1 - tp) * GROUP, GROUP), GROUP)
    mine = pl.ds(pl.multiple_of(tp * GROUP, GROUP), GROUP)
    tp_copies = []
    for i in range(share):
        w_copies[i].wait()
        y_buf[i] = lax.dot_general(lhs[...], w_buf[i], (((1,), (1,)), ((), ())), preferred_element_type=jnp.float32)
        c = remote(y_buf.at[i, theirs], from_tp.at[i], tp_send.at[i], tp_recv.at[i], across_y)
        c.start()
        tp_copies.append(c)

    started = []

    def piece(t, x, block):
        return gather.at[block, pl.ds(pl.multiple_of(x * 2 * GROUP + t * GROUP, GROUP), GROUP)]

    def send(ref, slot, i, peer):
        c = remote(ref, ref, ag_send.at[slot, i], ag_recv.at[slot, i], peer)
        c.start()
        started.append(c)

    def arrived(ref, slot, i):
        remote(ref, ref, ag_send.at[slot, i], ag_recv.at[slot, i], sibling).wait_recv()

    block = [share * core + i for i in range(share)]
    for i in range(share):
        tp_copies[i].wait_recv()
        gather[block[i], pl.ds(pl.multiple_of(chip * 2 * GROUP + tp * GROUP, GROUP), GROUP), :] = y_buf[i, mine] + from_tp[i] + bias[block[i]]
        ref = piece(tp, chip, block[i])
        send(ref, 1, i, across_y)
        send(ref, 0, i, across_x)
        send(ref, 4, i, sibling)
    for i in range(share):
        if i < share - 1:
            arrived(piece(1 - tp, chip, block[i]), 1, i)
            send(piece(1 - tp, chip, block[i]), 2, i, across_x)
            arrived(piece(tp, 1 - chip, block[i]), 0, i)
        else:
            arrived(piece(tp, 1 - chip, block[i]), 0, i)
            send(piece(tp, 1 - chip, block[i]), 2, i, across_y)
            arrived(piece(1 - tp, chip, block[i]), 1, i)
        send(piece(1 - tp, chip, block[i]), 6, i, sibling)
        send(piece(tp, 1 - chip, block[i]), 5, i, sibling)

    def turn(b):
        y_out[pl.ds(pl.multiple_of(b * width, width), width), :] = gather[b].T

    for i in range(share):
        arrived(piece(1 - tp, 1 - chip, block[i]), 2, i)
        send(piece(1 - tp, 1 - chip, block[i]), 3, i, sibling)
        turn(block[i])
    for i in range(share):
        other = share * (1 - core) + i
        arrived(piece(tp, chip, other), 4, i)
        arrived(piece(tp, 1 - chip, other), 5, i)
        arrived(piece(1 - tp, chip, other), 6, i)
        arrived(piece(1 - tp, 1 - chip, other), 3, i)
        turn(other)
    for c in core_copies + chip_copies + o_copies + tp_copies + started:
        c.wait_send()


def exchange(part, q_buf, k_out, v_out, seq_lens, sink_logits, w_o, bias):
    heads, d_out = w_o.shape
    n_col = bias.shape[0]
    cols = d_out // n_col
    share = n_col // 2
    hbm = lambda a: pltpu.with_memory_space_constraint(a, pltpu.HBM)
    vmem = pl.BlockSpec(memory_space=pltpu.VMEM)
    anyw = pl.BlockSpec(memory_space=pltpu.HBM)
    block = part.shape[1:]
    dma = pltpu.SemaphoreType.DMA
    return pl.pallas_call(
        exchange_kernel,
        out_shape=jax.ShapeDtypeStruct((d_out, 128), jnp.float32),
        in_specs=[vmem, vmem, anyw, anyw, anyw, anyw, vmem, anyw],
        out_specs=vmem,
        scratch_shapes=[
            pltpu.SMEM(seq_lens.shape, jnp.int32),
            pltpu.SMEM(sink_logits.shape, jnp.float32),
            pltpu.VMEM((2 * GROUP,) + k_out.shape[1:], jnp.bfloat16),
            pltpu.VMEM((2 * GROUP,) + k_out.shape[1:], jnp.bfloat16),
            pltpu.VMEM((2, GROUP * 32, 128), jnp.bfloat16),
            pltpu.VMEM((2,) + block, jnp.float32),
            pltpu.VMEM((share, cols, heads), jnp.bfloat16),
            pltpu.VMEM((2,) + block, jnp.float32),
            pltpu.VMEM(block, jnp.float32),
            pltpu.VMEM(block, jnp.float32),
            pltpu.VMEM(block, jnp.float32),
            pltpu.VMEM((2, 2, 256, 128), jnp.float32),
            pltpu.VMEM((2 * GROUP, heads), jnp.bfloat16),
            pltpu.VMEM((share, 2 * GROUP, cols), jnp.float32),
            pltpu.VMEM((share, GROUP, cols), jnp.float32),
            pltpu.VMEM((n_col, 128, cols), jnp.float32),
            dma((2,)), dma((2, 2)), dma((share,)), dma((5,)), dma((5,)), dma((4,)), dma((4,)), dma((4,)), dma((4,)), dma((share,)), dma((share,)),
            dma((7, share)), dma((7, share)),
        ],
        compiler_params=pltpu.CompilerParams(collective_id=0, has_side_effects=True, vmem_limit_bytes=40 * 1024 * 1024),
        cost_estimate=pl.CostEstimate(flops=4 * 10**8, bytes_accessed=16 * 10**6, transcendentals=10**5),
      )(part, q_buf, hbm(k_out), hbm(v_out), hbm(seq_lens), hbm(sink_logits), bias, hbm(w_o.T))


def solution(mesh):
    cache_spec = P("dp", "sp", "tp", None)

    def block_step(hidden, seq_lens, rope_cos, rope_sin, k_cache, v_cache, norm_gain, w_qkv, b_qkv, sink_logits, w_o, b_o):
        d_model = hidden.shape[1]
        gain = norm_gain.astype(jnp.float32).reshape(PARTS, 1, d_model // PARTS)
        bias = b_o.astype(jnp.float32).reshape(BLOCKS, 1, d_model // BLOCKS)
        k_out, v_out, part, q_buf = local_attention(hidden, seq_lens, rope_cos, rope_sin, k_cache, v_cache, gain, w_qkv, b_qkv, sink_logits)
        y_t = exchange(part, q_buf, k_out, v_out, seq_lens, sink_logits, w_o, bias)
        out_hidden = (hidden.T.astype(jnp.float32) + y_t).astype(jnp.bfloat16).T
        seqs, ctx, kv, dim = k_cache.shape
        back = lambda a: a.reshape(seqs, kv, dim, ctx).transpose(0, 3, 1, 2)
        return out_hidden, back(k_out), back(v_out)

    return jax.shard_map(block_step, mesh=mesh, in_specs=(P("dp", None), P("dp"), P("dp", None), P("dp", None), cache_spec, cache_spec, P(None), P(None, "tp", None), P("tp", None), P("tp"), P("tp", None), P(None)), out_specs=(P("dp", None), cache_spec, cache_spec), check_vma=False)
```
